128 devices in a mesh: sector: 16 (over y, x_lo, core), row: 8 (over z, x_hi).
Axes of the slice: x: 4 (x_hi: 2, x_lo: 2; x = x_hi * 2 + x_lo), y: 4, z: 4, core: 2. Of those that a mesh axis runs over, the one named last changes fastest.
Arguments:
- psi_sectors: bfloat16 [64, 16384, 256], P('sector', 'row'), may hold values from -1.25 to 1.25
- stiff_blocks: bfloat16 [128, 5, 128, 128], P('row'), as said below
- mass_blocks: bfloat16 [128, 5, 128, 128], P('row'), as said below
- harmonic_table: int32 [32], replicated, may hold values from 0 to 31, each once
Outputs:
- reduced_stiffness: float32 [32, 512, 512], P('sector', 'row')
- reduced_mass: float32 [32, 512, 512], P('sector', 'row')
The draws below stay inside these ranges and needn't reach their ends.
Inputs may be any that keep to these rules, and one draw needn't show every extreme that they name: The stiffness is symmetric: stiff_blocks[i, 2 + d] is the transpose of stiff_blocks[i + d, 2 - d], and blocks whose column lies outside 0 to 127 are zero. `mass_blocks`: the mass is symmetric in the same way, and diagonally dominant with a positive diagonal, hence positive definite.
All inputs are finite; a program needn't handle non-finite values.
Results may differ from the reference program's by a relative error of at most 0.0049.
Values may be sent and summed in bfloat16 or wider, within the bound.
A program may use at most 128 MiB of HBM per device.

```python
import math
import jax
import jax.numpy as jnp
from jax import lax

M = 256
B = 128
REACH = 2
NBAND = 5
SECTORS = 64
SLOTS = 32
DOF = 16384
NBLK = 128


def build_band(key, entry_scale):
    upper_part = jnp.clip(jax.random.normal(key, (NBLK, REACH + 1, B, B), jnp.float32), -6.0, 6.0) * entry_scale
    middle = (upper_part[:, 0] + jnp.swapaxes(upper_part[:, 0], 1, 2)) * 0.5 ** 0.5
    block_ids = jnp.arange(NBLK, dtype=jnp.int32)[:, None, None]
    columns = []
    for offset in range(-REACH, REACH + 1):
        if offset == 0:
            columns.append(middle)
        elif offset > 0:
            inside = block_ids + offset < NBLK
            columns.append(jnp.where(inside, upper_part[:, offset], 0.0))
        else:
            distance = -offset
            flipped = jnp.swapaxes(upper_part[:, distance], 1, 2)
            shifted = jnp.concatenate([jnp.zeros((distance, B, B), jnp.float32), flipped[:NBLK - distance]], axis=0)
            columns.append(shifted)
    return jnp.stack(columns, axis=1)


def draw_stiff_blocks(key, part):
    band = build_band(jax.random.fold_in(key, 11), (NBAND * B) ** (-0.5))
    return band.astype(jnp.bfloat16)


def draw_mass_blocks(key, part):
    band = build_band(jax.random.fold_in(key, 23), 1.0 / (NBAND * B))
    identity = jnp.eye(B, dtype=jnp.float32)
    own_diagonal = jnp.abs(jnp.diagonal(band[:, REACH], axis1=1, axis2=2))
    off_sum = jnp.sum(jnp.abs(band), axis=(1, 3)) - own_diagonal
    factor = jax.random.uniform(jax.random.fold_in(key, 29), (NBLK, B), jnp.float32, 1.1, 2.0)
    new_diagonal = off_sum * factor
    centre = band[:, REACH] * (1.0 - identity) + new_diagonal[:, :, None] * identity
    band = band.at[:, REACH].set(centre)
    return band.astype(jnp.bfloat16)


def block_scale(key, dims, cuts, smallest, largest):
    level = 1.0
    for position, parts in cuts:
        steps = jax.random.uniform(jax.random.fold_in(jax.random.fold_in(key, 6), position), (parts,), jnp.float32, smallest / len(cuts), largest / len(cuts))
        level = level * jnp.repeat(jnp.exp(steps), dims[position] // parts).reshape((-1,) + (1,) * (len(dims) - 1 - position))
    return level


def gaussian(rng, extent, spread, reach, split=(), kind=jnp.bfloat16):
    entries = jax.random.normal(rng, extent, jnp.float32) * spread
    if len(split) > 0:
        entries = block_scale(rng, extent, split, -0.22, 0.18) * entries
    return jnp.clip(entries, min=-reach, max=reach).astype(kind)


def setup_inputs(seed: int = 0) -> dict:
    streams_of = jax.random.split(jax.random.key(seed), 5)
    return {
        "psi_sectors": gaussian(streams_of[0], (SECTORS, DOF, M), (DOF ** -0.25), 1.25, ((0, 16), (1, 8))),
        "stiff_blocks": draw_stiff_blocks(jax.random.fold_in(streams_of[4], 71), 0),
        "mass_blocks": draw_mass_blocks(jax.random.fold_in(streams_of[4], 71), 0),
        "harmonic_table": jax.random.permutation(streams_of[3], SLOTS).astype(jnp.int32),
    }


def coefficients(harmonic_table, sectors_all):
    sector_ids = jnp.arange(sectors_all, dtype=jnp.int32)
    pair_table = harmonic_table.astype(jnp.int32)
    half_count = sectors_all // 2
    second_freq = jnp.where(pair_table == 0, half_count, pair_table)
    first_phase = pair_table[:, None] * sector_ids[None, :] % sectors_all
    second_phase = second_freq[:, None] * sector_ids[None, :] % sectors_all
    angle_unit = 2.0 * math.pi / sectors_all
    first_angle = first_phase.astype(jnp.float32) * angle_unit
    second_angle = second_phase.astype(jnp.float32) * angle_unit
    zero_pair = (pair_table == 0)[:, None]
    low_scale = math.sqrt(1.0 / sectors_all)
    high_scale = math.sqrt(2.0 / sectors_all)
    first_row = jnp.where(zero_pair, low_scale, high_scale) * jnp.cos(first_angle)
    second = jnp.where(zero_pair, low_scale * jnp.cos(second_angle), high_scale * jnp.sin(second_angle))
    return jnp.stack([first_row, second], axis=1).reshape(2 * pair_table.shape[0], sectors_all)

def band_apply(blocks, harmonic):
    block_rows = blocks.shape[0]
    band_count = blocks.shape[1]
    padded = jnp.pad(harmonic.reshape(block_rows, B, harmonic.shape[1]), ((REACH, REACH), (0, 0), (0, 0)))
    block_index = jnp.arange(block_rows, dtype=jnp.int32)[:, None] + jnp.arange(band_count, dtype=jnp.int32)[None, :]
    gathered = padded[block_index].astype(jnp.float32)
    images = jnp.einsum('ijab,ijbm->iam', blocks.astype(jnp.float32), gathered)
    return images.reshape(harmonic.shape).astype(jnp.bfloat16)

def reference(psi_sectors, stiff_blocks, mass_blocks, harmonic_table):
    sectors_all = psi_sectors.shape[0]
    dof_count = psi_sectors.shape[1]
    mode_count = psi_sectors.shape[2]
    dft_table = coefficients(harmonic_table, sectors_all)
    flattened = psi_sectors.reshape(sectors_all, dof_count * mode_count).astype(jnp.float32)
    harmonics = jnp.dot(dft_table, flattened, precision=lax.Precision.HIGHEST).astype(jnp.bfloat16)
    harmonics = harmonics.reshape(sectors_all // 2, 2, dof_count, mode_count)

    def one_slot(pair_field):
        left_basis = jnp.concatenate([pair_field[0], pair_field[1]], axis=1)
        stiff_wide = jnp.concatenate([band_apply(stiff_blocks, pair_field[0]), band_apply(stiff_blocks, pair_field[1])], axis=1)
        mass_wide = jnp.concatenate([band_apply(mass_blocks, pair_field[0]), band_apply(mass_blocks, pair_field[1])], axis=1)
        return (jnp.dot(left_basis.T, stiff_wide, preferred_element_type=jnp.float32), jnp.dot(left_basis.T, mass_wide, preferred_element_type=jnp.float32))
    reduced_stiffness, reduced_mass = lax.map(one_slot, harmonics)
    return (reduced_stiffness, reduced_mass)
```

```python
import functools
import math

import jax
import jax.numpy as jnp
from jax import lax
from jax.experimental import pallas as pl
from jax.experimental.pallas import tpu as pltpu
from jax.sharding import PartitionSpec as P

MESH = pl.DeviceIdType.MESH
B = 128
M = 256
NBAND = 5
ROWS_DEV = 2048
SEG = 1024
CHUNK = 256
NCHUNK = 4
PIECE = 32
TILE = 16
SLOTS_DEV = 4
ORDER = (3, 0, 1, 2)
HALO = 256
SECTOR_OFFSETS = tuple(
    (dy, dx, dc) for dy in (2, 1, 3, 0) for dx in (1, 0) for dc in (0, 1) if dy or dx or dc
)
OWNER_OFFSETS = tuple((dy, dc) for dy in (2, 1, 3, 0) for dc in (0, 1) if dy or dc)


def coefficients(harmonic_table, sectors_all):
    sector_ids = jnp.arange(sectors_all, dtype=jnp.int32)
    half_count = sectors_all // 2
    second_freq = jnp.where(harmonic_table == 0, half_count, harmonic_table)
    first_phase = harmonic_table[:, None] * sector_ids[None, :] % sectors_all
    second_phase = second_freq[:, None] * sector_ids[None, :] % sectors_all
    angle_unit = 2.0 * math.pi / sectors_all
    first_angle = first_phase.astype(jnp.float32) * angle_unit
    second_angle = second_phase.astype(jnp.float32) * angle_unit
    zero_pair = (harmonic_table == 0)[:, None]
    low_scale = math.sqrt(1.0 / sectors_all)
    high_scale = math.sqrt(2.0 / sectors_all)
    first_row = jnp.where(zero_pair, low_scale, high_scale) * jnp.cos(first_angle)
    second = jnp.where(
        zero_pair, low_scale * jnp.cos(second_angle), high_scale * jnp.sin(second_angle)
    )
    return jnp.concatenate([first_row, second], axis=0)


def kernel(
    psi, stiff, mass, table, out_k, out_m,
    arrived, sent, fields, lift, bands, images, total, parts, pieces,
    load_sem, s1, r1, s2, r2, sh, rh, s3, r3,
):
    sec = lax.axis_index("sector")
    row = lax.axis_index("row")
    y, xl, core = sec // 4, (sec // 2) % 2, sec % 2
    turn = y * 2 + core
    seg = row * 2 + xl

    def device(y_, xl_, core_, row_):
        return {"sector": y_ * 4 + xl_ * 2 + core_, "row": row_}

    loads = []
    for m, src in enumerate((stiff, mass)):
        for k in range(NBAND):
            copy = pltpu.make_async_copy(
                src.at[pl.ds(pl.multiple_of(xl * 8, 8), 8), k],
                bands.at[:, pl.ds(m * B, B), pl.ds(k * B, B)],
                load_sem.at[m, k],
            )
            copy.start()
            loads.append(copy)

    barrier = pltpu.get_barrier_semaphore()
    count = 0
    for dy, dx, dc in SECTOR_OFFSETS:
        pl.semaphore_signal(
            barrier, inc=1, device_id_type=MESH,
            device_id=device((y + dy) % 4, (xl + dx) % 2, (core + dc) % 2, row),
        )
        count += 1
    for dr in range(1, 8):
        for dx in range(2):
            pl.semaphore_signal(
                barrier, inc=1, device_id_type=MESH,
                device_id=device(y, (xl + dx) % 2, core, (row + dr) % 8),
            )
            count += 1
    pl.semaphore_wait(barrier, count)

    def rows_of(xl_, turn_, q):
        return pl.ds(pl.multiple_of(xl_ * SEG + q * CHUNK + turn_ * PIECE, PIECE), PIECE)

    for q in ORDER:
        for dy, dx, dc in SECTOR_OFFSETS:
            y_, xl_, core_ = (y + dy) % 4, (xl + dx) % 2, (core + dc) % 2
            pltpu.make_async_remote_copy(
                src_ref=psi.at[:, rows_of(xl_, y_ * 2 + core_, q), :],
                dst_ref=arrived.at[q, pl.ds(sec * 4, 4)],
                send_sem=s1.at[q],
                recv_sem=r1.at[q],
                device_id=device(y_, xl_, core_, row),
                device_id_type=MESH,
            ).start()
        pltpu.make_async_copy(
            psi.at[:, rows_of(xl, turn, q), :], arrived.at[q, pl.ds(sec * 4, 4)], r1.at[q]
        ).start()

    coef = table[...]
    coef_hi = coef.astype(jnp.bfloat16)
    coef_lo = (coef - coef_hi.astype(jnp.float32)).astype(jnp.bfloat16)
    quarter = 256

    def spread(n, _):
        i = lax.broadcasted_iota(jnp.int32, (quarter, 64), 0) + n * quarter
        g = i // TILE
        e, t, k = g % 2, (g // 2) % 8, g // 16
        slot = (t // 2) * 8 + (k // 2) * 4 + (t % 2) * 2 + k % 2
        want = e * 32 + slot
        pick = (lax.broadcasted_iota(jnp.int32, (quarter, 64), 1) == want).astype(jnp.bfloat16)
        col = lax.broadcasted_iota(jnp.int32, (64, 1024), 1) // TILE
        wide = (lax.broadcasted_iota(jnp.int32, (64, 1024), 0) == col).astype(jnp.bfloat16)
        same = (
            lax.broadcasted_iota(jnp.int32, (quarter, 1024), 0) % TILE
            == lax.broadcasted_iota(jnp.int32, (quarter, 1024), 1) % TILE
        )
        for h, part in enumerate((coef_hi, coef_lo)):
            chosen = jnp.dot(pick, part, preferred_element_type=jnp.float32).astype(jnp.bfloat16)
            full = jnp.dot(chosen, wide, preferred_element_type=jnp.float32)
            lift[h, pl.ds(pl.multiple_of(n * quarter, quarter), quarter), :] = jnp.where(
                same, full, 0.0
            ).astype(jnp.bfloat16)
        return 0

    lax.fori_loop(0, 4, spread, 0)

    def send_fields(k, q):
        mine = pl.ds(pl.multiple_of(HALO + q * CHUNK + turn * PIECE, PIECE), PIECE)
        for dy, dc in OWNER_OFFSETS:
            y_, core_ = (y + dy) % 4, (core + dc) % 2
            pltpu.make_async_remote_copy(
                src_ref=sent.at[q, pl.ds(k * 16 + (y_ * 2 + core_) * 2, 2)],
                dst_ref=fields.at[k, :, mine, :],
                send_sem=s2.at[k],
                recv_sem=r2.at[k, q],
                device_id=device(y_, xl, core_, row),
                device_id_type=MESH,
            ).start()
        pltpu.make_async_copy(
            sent.at[q, pl.ds(k * 16 + turn * 2, 2)], fields.at[k, :, mine, :], r2.at[k, q]
        ).start()

    for q in ORDER:
        pltpu.make_async_copy(arrived.at[q], arrived.at[q], r1.at[q]).wait()

        def transform(h, _):
            rows = pl.ds(pl.multiple_of(h * TILE, TILE), TILE)
            x = arrived[q, :, rows, :].reshape(64 * TILE, M)
            for n in range(2):
                at = pl.ds(n * 512, 512)
                out = jnp.dot(lift[0, at, :], x, preferred_element_type=jnp.float32)
                out += jnp.dot(lift[1, at, :], x, preferred_element_type=jnp.float32)
                sent[q, pl.ds(n * 32, 32), rows, :] = out.astype(jnp.bfloat16).reshape(
                    32, TILE, M
                )
            return 0

        lax.fori_loop(0, PIECE // TILE, transform, 0)
        send_fields(0, q)

    for copy in loads:
        copy.wait()

    def process(k, q, first):
        for b in range(2):
            i = 2 * q + b
            for e in range(2):
                window = fields[k, e, pl.ds(i * B, NBAND * B), :]
                w = jnp.dot(bands[i], window, preferred_element_type=jnp.float32)
                w = w.astype(jnp.bfloat16)
                images[pl.ds(b * B, B), pl.ds(e * M, M)] = w[:B]
                images[pl.ds(b * B, B), pl.ds(2 * M + e * M, M)] = w[B:]
        for e in range(2):
            left = fields[k, e, pl.ds(HALO + q * CHUNK, CHUNK), :]
            part = lax.dot_general(
                left, images[...], (((0,), (0,)), ((), ())), preferred_element_type=jnp.float32
            )
            at = pl.ds(e * M, M)
            if first:
                total[at, :] = part
            else:
                total[at, :] += part

    def arrival(k, q):
        whole = fields.at[k, :, pl.ds(0, CHUNK), :]
        pltpu.make_async_copy(whole, whole, r2.at[k, q]).wait()

    def halo(k, up):
        to = (seg + (1 if up else 15)) % 16
        src, dst = (SEG, 0) if up else (HALO, HALO + SEG)
        side = 0 if up else 1
        return pltpu.make_async_remote_copy(
            src_ref=fields.at[k, :, pl.ds(src, HALO), :],
            dst_ref=fields.at[k, :, pl.ds(dst, HALO), :],
            send_sem=sh.at[k, side],
            recv_sem=rh.at[k, side],
            device_id=device(y, to % 2, core, to // 2),
            device_id_type=MESH,
        )

    def slot(k):
        if k + 1 < SLOTS_DEV:
            for q in ORDER:
                send_fields(k + 1, q)
        arrival(k, 3)
        halo(k, True).start()
        arrival(k, 0)
        halo(k, False).start()
        arrival(k, 1)
        halo(k, True).wait_recv()
        process(k, 0, True)
        arrival(k, 2)
        process(k, 1, False)
        process(k, 2, False)
        halo(k, False).wait_recv()
        process(k, 3, False)
        parts[k] = total[...].astype(jnp.bfloat16)
        owner = k // 2
        for dr in (4, 5, 3, 6, 2, 7, 1):
            row_ = (row + dr) % 8
            pltpu.make_async_remote_copy(
                src_ref=parts.at[k, pl.ds(pl.multiple_of(row_ * 64, 64), 64), :],
                dst_ref=pieces.at[k % 2, seg],
                send_sem=s3.at[k, 0],
                recv_sem=r3.at[k % 2],
                device_id=device(y, owner, core, row_),
                device_id_type=MESH,
            ).start()
        own = parts.at[k, pl.ds(pl.multiple_of(row * 64, 64), 64), :]

        @pl.when(xl == owner)
        def _():
            pltpu.make_async_copy(own, pieces.at[k % 2, seg], r3.at[k % 2]).start()

        @pl.when(xl != owner)
        def _():
            pltpu.make_async_remote_copy(
                src_ref=own,
                dst_ref=pieces.at[k % 2, seg],
                send_sem=s3.at[k, 1],
                recv_sem=r3.at[k % 2],
                device_id=device(y, 1 - xl, core, row),
                device_id_type=MESH,
            ).start()

    for k in range(SLOTS_DEV):
        slot(k)

    for k in range(2):
        pltpu.make_async_copy(pieces.at[k], pieces.at[k], r3.at[k]).wait()
        acc = pieces[k, 0].astype(jnp.float32)
        for n in range(1, 16):
            acc += pieces[k, n].astype(jnp.float32)
        out_k[k] = acc[:, :512]
        out_m[k] = acc[:, 512:]

    for q in range(NCHUNK):
        gone = arrived.at[q, pl.ds(0, 60)]
        pltpu.make_async_copy(gone, gone, s1.at[q]).wait()
    for k in range(SLOTS_DEV):
        gone = sent.at[pl.ds(0, 4), pl.ds(0, 14)]
        pltpu.make_async_copy(gone, gone, s2.at[k]).wait()
        halo(k, True).wait_send()
        halo(k, False).wait_send()
        gone = parts.at[k, pl.ds(0, 448), :]
        pltpu.make_async_copy(gone, gone, s3.at[k, 0]).wait()

        @pl.when(xl != k // 2)
        def _():
            gone = parts.at[k, pl.ds(0, 64), :]
            pltpu.make_async_copy(gone, gone, s3.at[k, 1]).wait()


def per_device(psi_sectors, stiff_blocks, mass_blocks, harmonic_table):
    table = coefficients(harmonic_table, 64)
    anywhere = pl.BlockSpec(memory_space=pl.ANY)
    vmem = pl.BlockSpec(memory_space=pltpu.VMEM)
    bf16, f32 = jnp.bfloat16, jnp.float32
    dma = pltpu.SemaphoreType.DMA
    return pl.pallas_call(
        kernel,
        out_shape=(
            jax.ShapeDtypeStruct((2, 64, 512), f32),
            jax.ShapeDtypeStruct((2, 64, 512), f32),
        ),
        in_specs=[anywhere, anywhere, anywhere, vmem],
        out_specs=(vmem, vmem),
        scratch_shapes=[
            pltpu.VMEM((NCHUNK, 64, PIECE, M), bf16),
            pltpu.VMEM((NCHUNK, 64, PIECE, M), bf16),
            pltpu.VMEM((SLOTS_DEV, 2, SEG + 2 * HALO, M), bf16),
            pltpu.VMEM((2, 1024, 1024), bf16),
            pltpu.VMEM((8, 2 * B, NBAND * B), bf16),
            pltpu.VMEM((CHUNK, 4 * M), bf16),
            pltpu.VMEM((2 * M, 4 * M), f32),
            pltpu.VMEM((SLOTS_DEV, 2 * M, 4 * M), bf16),
            pltpu.VMEM((2, 16, 64, 4 * M), bf16),
            dma((2, NBAND)),
            dma((NCHUNK,)),
            dma((NCHUNK,)),
            dma((SLOTS_DEV,)),
            dma((SLOTS_DEV, NCHUNK)),
            dma((SLOTS_DEV, 2)),
            dma((SLOTS_DEV, 2)),
            dma((SLOTS_DEV, 2)),
            dma((2,)),
        ],
        compiler_params=pltpu.CompilerParams(
            collective_id=0, has_side_effects=True, vmem_limit_bytes=60 * 1024 * 1024
        ),
        name="reduce_sectors",
    )(psi_sectors, stiff_blocks, mass_blocks, table)


def solution(mesh):
    placed = (P("sector", "row", None), P("row", None, None, None), P("row", None, None, None), P())
    return jax.shard_map(
        per_device,
        mesh=mesh,
        in_specs=placed,
        out_specs=(P("sector", "row", None), P("sector", "row", None)),
        check_vma=False,
    )
```

```python
import functools
import math

import jax
import jax.numpy as jnp
from jax import lax
from jax.experimental import pallas as pl
from jax.experimental.pallas import tpu as pltpu
from jax.sharding import PartitionSpec as P

MESH = pl.DeviceIdType.MESH
B = 128
M = 256
NBAND = 5
ROWS_DEV = 2048
SEG = 1024
CHUNK = 256
NCHUNK = 4
PIECE = 32
TILE = 16
SLOTS_DEV = 4
ORDER = (3, 0, 1, 2)
HALO = 256
SECTORS = 64
SLOTS = 32
SECTOR_OFFSETS = tuple(
    (dy, dx, dc) for dy in (2, 1, 3, 0) for dx in (1, 0) for dc in (0, 1) if dy or dx or dc
)
OWNER_OFFSETS = tuple((dy, dc) for dy in (2, 1, 3, 0) for dc in (0, 1) if dy or dc)


def coefficients(table):
    shape = (2 * SLOTS, SECTORS)
    line = lax.broadcasted_iota(jnp.int32, shape, 0)
    sector = lax.broadcasted_iota(jnp.int32, shape, 1)
    pair = jnp.zeros(shape, jnp.int32)
    for j in range(SLOTS):
        pair = jnp.where(line % SLOTS == j, table[j], pair)
    first = line < SLOTS
    zero = pair == 0
    freq = jnp.where(jnp.logical_and(zero, jnp.logical_not(first)), SECTORS // 2, pair)
    shift = jnp.where(jnp.logical_or(first, zero), 0, 3 * SECTORS // 4)
    phase = (freq * sector + shift) % SECTORS
    wave = jnp.cos(phase.astype(jnp.float32) * (2.0 * math.pi / SECTORS))
    return jnp.where(zero, math.sqrt(1.0 / SECTORS), math.sqrt(2.0 / SECTORS)) * wave


def kernel(
    psi, stiff, mass, table, out_k, out_m,
    arrived, sent, fields, lift, bands, images, total, parts, stage, middle, pieces, last,
    load_sem, s1, r1, s2, r2, sh, rh, s3, r3, s4, r4, s5, r5,
):
    sec = lax.axis_index("sector")
    row = lax.axis_index("row")
    y, xl, core = sec // 4, (sec // 2) % 2, sec % 2
    turn = y * 2 + core
    seg = row * 2 + xl
    z, xh = row // 2, row % 2

    def device(y_, xl_, core_, row_):
        return {"sector": y_ * 4 + xl_ * 2 + core_, "row": row_}

    loads = []
    for m, src in enumerate((stiff, mass)):
        for k in range(NBAND):
            copy = pltpu.make_async_copy(
                src.at[pl.ds(pl.multiple_of(xl * 8, 8), 8), k],
                bands.at[:, pl.ds(m * B, B), pl.ds(k * B, B)],
                load_sem.at[m, k],
            )
            copy.start()
            loads.append(copy)

    barrier = pltpu.get_barrier_semaphore()
    count = 0
    for dy, dx, dc in SECTOR_OFFSETS:
        pl.semaphore_signal(
            barrier, inc=1, device_id_type=MESH,
            device_id=device((y + dy) % 4, (xl + dx) % 2, (core + dc) % 2, row),
        )
        count += 1
    for dr in range(1, 8):
        for dx in range(2):
            pl.semaphore_signal(
                barrier, inc=1, device_id_type=MESH,
                device_id=device(y, (xl + dx) % 2, core, (row + dr) % 8),
            )
            count += 1
    with jax.named_scope("barrier"):
        pl.semaphore_wait(barrier, count)

    def rows_of(xl_, turn_, q):
        return pl.ds(pl.multiple_of(xl_ * SEG + q * CHUNK + turn_ * PIECE, PIECE), PIECE)

    for q in ORDER:
        for dy, dx, dc in SECTOR_OFFSETS:
            y_, xl_, core_ = (y + dy) % 4, (xl + dx) % 2, (core + dc) % 2
            pltpu.make_async_remote_copy(
                src_ref=psi.at[:, rows_of(xl_, y_ * 2 + core_, q), :],
                dst_ref=arrived.at[q, pl.ds(sec * 4, 4)],
                send_sem=s1.at[q],
                recv_sem=r1.at[q],
                device_id=device(y_, xl_, core_, row),
                device_id_type=MESH,
            ).start()
        pltpu.make_async_copy(
            psi.at[:, rows_of(xl, turn, q), :], arrived.at[q, pl.ds(sec * 4, 4)], r1.at[q]
        ).start()

    coef = coefficients(table)
    coef_hi = coef.astype(jnp.bfloat16)
    coef_lo = (coef - coef_hi.astype(jnp.float32)).astype(jnp.bfloat16)
    quarter = 256

    def spread(n, _):
        i = lax.broadcasted_iota(jnp.int32, (quarter, 64), 0) + n * quarter
        g = i // TILE
        e, t, k = g % 2, (g // 2) % 8, g // 16
        slot = (t // 2) * 8 + ((k // 2 + t) % 2) * 4 + (t % 2) * 2 + k % 2
        want = e * 32 + slot
        pick = (lax.broadcasted_iota(jnp.int32, (quarter, 64), 1) == want).astype(jnp.bfloat16)
        col = lax.broadcasted_iota(jnp.int32, (64, 1024), 1) // TILE
        wide = (lax.broadcasted_iota(jnp.int32, (64, 1024), 0) == col).astype(jnp.bfloat16)
        same = (
            lax.broadcasted_iota(jnp.int32, (quarter, 1024), 0) % TILE
            == lax.broadcasted_iota(jnp.int32, (quarter, 1024), 1) % TILE
        )
        for h, part in enumerate((coef_hi, coef_lo)):
            chosen = jnp.dot(pick, part, preferred_element_type=jnp.float32).astype(jnp.bfloat16)
            full = jnp.dot(chosen, wide, preferred_element_type=jnp.float32)
            lift[h, pl.ds(pl.multiple_of(n * quarter, quarter), quarter), :] = jnp.where(
                same, full, 0.0
            ).astype(jnp.bfloat16)
        return 0

    with jax.named_scope("spread"):
        lax.fori_loop(0, 4, spread, 0)

    def send_fields(k, q):
        mine = pl.ds(pl.multiple_of(HALO + q * CHUNK + turn * PIECE, PIECE), PIECE)
        for dy, dc in OWNER_OFFSETS:
            y_, core_ = (y + dy) % 4, (core + dc) % 2
            pltpu.make_async_remote_copy(
                src_ref=sent.at[q, pl.ds(k * 16 + (y_ * 2 + core_) * 2, 2)],
                dst_ref=fields.at[k, :, mine, :],
                send_sem=s2.at[k],
                recv_sem=r2.at[k, q],
                device_id=device(y_, xl, core_, row),
                device_id_type=MESH,
            ).start()
        pltpu.make_async_copy(
            sent.at[q, pl.ds(k * 16 + turn * 2, 2)], fields.at[k, :, mine, :], r2.at[k, q]
        ).start()

    for q in ORDER:
        with jax.named_scope(f"wait_one#q={q}"):
            pltpu.make_async_copy(arrived.at[q], arrived.at[q], r1.at[q]).wait()

        def transform(h, _):
            rows = pl.ds(pl.multiple_of(h * TILE, TILE), TILE)
            x = arrived[q, :, rows, :].reshape(64 * TILE, M)
            for n in range(2):
                at = pl.ds(n * 512, 512)
                out = jnp.dot(lift[0, at, :], x, preferred_element_type=jnp.float32)
                out += jnp.dot(lift[1, at, :], x, preferred_element_type=jnp.float32)
                sent[q, pl.ds(n * 32, 32), rows, :] = out.astype(jnp.bfloat16).reshape(
                    32, TILE, M
                )
            return 0

        with jax.named_scope(f"transform#q={q}"):
            lax.fori_loop(0, PIECE // TILE, transform, 0)
        send_fields(0, q)

    for copy in loads:
        copy.wait()

    def process(k, q, first):
        for b in range(2):
            i = 2 * q + b
            for e in range(2):
                window = fields[k, e, pl.ds(i * B, NBAND * B), :]
                w = jnp.dot(bands[i], window, preferred_element_type=jnp.float32)
                w = w.astype(jnp.bfloat16)
                images[pl.ds(b * B, B), pl.ds(e * M, M)] = w[:B]
                images[pl.ds(b * B, B), pl.ds(2 * M + e * M, M)] = w[B:]
        for e in range(2):
            left = fields[k, e, pl.ds(HALO + q * CHUNK, CHUNK), :]
            part = lax.dot_general(
                left, images[...], (((0,), (0,)), ((), ())), preferred_element_type=jnp.float32
            )
            at = pl.ds(e * M, M)
            if first:
                total[at, :] = part
            else:
                total[at, :] += part

    def arrival(k, q):
        whole = fields.at[k, :, pl.ds(0, CHUNK), :]
        with jax.named_scope(f"wait_two#k={k}#q={q}"):
            pltpu.make_async_copy(whole, whole, r2.at[k, q]).wait()

    def halo(k, up):
        to = (seg + (1 if up else 15)) % 16
        src, dst = (SEG, 0) if up else (HALO, HALO + SEG)
        side = 0 if up else 1
        return pltpu.make_async_remote_copy(
            src_ref=fields.at[k, :, pl.ds(src, HALO), :],
            dst_ref=fields.at[k, :, pl.ds(dst, HALO), :],
            send_sem=sh.at[k, side],
            recv_sem=rh.at[k, side],
            device_id=device(y, to % 2, core, to // 2),
            device_id_type=MESH,
        )

    def slot(k):
        if k + 2 < SLOTS_DEV:
            for q in ORDER:
                send_fields(k + 2, q)
        arrival(k, 3)
        halo(k, True).start()
        arrival(k, 0)
        halo(k, False).start()
        arrival(k, 1)
        with jax.named_scope(f"wait_low#k={k}"):
            halo(k, True).wait_recv()
        with jax.named_scope(f"process#k={k}#q=0"):
            process(k, 0, True)
        arrival(k, 2)
        with jax.named_scope(f"process#k={k}#q=1"):
            process(k, 1, False)
        with jax.named_scope(f"process#k={k}#q=2"):
            process(k, 2, False)
        with jax.named_scope(f"wait_high#k={k}"):
            halo(k, False).wait_recv()
        with jax.named_scope(f"process#k={k}#q=3"):
            process(k, 3, False)
        with jax.named_scope(f"narrow#k={k}"):
            parts[k] = total[...].astype(jnp.bfloat16)
        if k < SLOTS_DEV - 1:
            for dz in (2, 1, 3):
                column(k, dz).start()
        else:
            for dr in (4, 5, 3, 6, 2, 7, 1):
                direct(dr).start()

            @pl.when(xl == owner(k))
            def _():
                pltpu.make_async_copy(direct_part(row), last.at[seg], r4).start()

            @pl.when(xl != owner(k))
            def _():
                direct(0).start()

    def owner(k):
        return (k // 2 + core) % 2

    def column(k, dz):
        z_ = (z + dz) % 4
        return pltpu.make_async_remote_copy(
            src_ref=parts.at[k, pl.ds(pl.multiple_of(z_ * 128, 128), 128), :],
            dst_ref=stage.at[k, (3 - dz)],
            send_sem=s3.at[k],
            recv_sem=r3.at[k],
            device_id=device(y, xl, core, z_ * 2 + xh),
            device_id_type=MESH,
        )

    def across(k, dh):
        xh_ = (xh + dh) % 2
        return pltpu.make_async_remote_copy(
            src_ref=middle.at[k, pl.ds(pl.multiple_of(xh_ * 64, 64), 64), :],
            dst_ref=pieces.at[k % 2, xh * 2 + xl],
            send_sem=s5.at[k, dh],
            recv_sem=r5.at[k % 2],
            device_id=device(y, owner(k), core, z * 2 + xh_),
            device_id_type=MESH,
        )

    def direct_part(row_):
        return parts.at[SLOTS_DEV - 1, pl.ds(pl.multiple_of(row_ * 64, 64), 64), :]

    def direct(dr):
        row_ = (row + dr) % 8
        return pltpu.make_async_remote_copy(
            src_ref=direct_part(row_),
            dst_ref=last.at[seg],
            send_sem=s4.at[0 if dr else 1],
            recv_sem=r4,
            device_id=device(y, owner(SLOTS_DEV - 1), core, row_),
            device_id_type=MESH,
        )

    def second(k):
        with jax.named_scope(f"wait_stage#k={k}"):
            pltpu.make_async_copy(stage.at[k], stage.at[k], r3.at[k]).wait()
        acc = parts[k, pl.ds(pl.multiple_of(z * 128, 128), 128), :].astype(jnp.float32)
        for n in range(3):
            acc += stage[k, n].astype(jnp.float32)
        middle[k] = acc.astype(jnp.bfloat16)
        across(k, 1).start()

        @pl.when(xl == owner(k))
        def _():
            pltpu.make_async_copy(
                middle.at[k, pl.ds(pl.multiple_of(xh * 64, 64), 64), :],
                pieces.at[k % 2, xh * 2 + xl],
                r5.at[k % 2],
            ).start()

        @pl.when(xl != owner(k))
        def _():
            across(k, 0).start()

    for q in ORDER:
        send_fields(1, q)
    for k in range(SLOTS_DEV):
        slot(k)
        if k:
            second(k - 1)

    def combine(k, src, count):
        acc = src[0].astype(jnp.float32)
        for n in range(1, count):
            acc += src[n].astype(jnp.float32)
        out_k[k] = acc[:, :512]
        out_m[k] = acc[:, 512:]

    def two_stage(k):
        with jax.named_scope(f"wait_pieces#k={k}"):
            pltpu.make_async_copy(pieces.at[k], pieces.at[k], r5.at[k]).wait()
        combine(k, pieces.at[k], 4)

    two_stage(0)

    @pl.when(xl == owner(0))
    def _():
        two_stage(1)

    @pl.when(xl != owner(0))
    def _():
        with jax.named_scope("wait_last"):
            pltpu.make_async_copy(last, last, r4).wait()
        combine(1, last, 16)

    for q in range(NCHUNK):
        gone = arrived.at[q, pl.ds(0, 60)]
        pltpu.make_async_copy(gone, gone, s1.at[q]).wait()
    for k in range(SLOTS_DEV):
        gone = sent.at[pl.ds(0, 4), pl.ds(0, 14)]
        pltpu.make_async_copy(gone, gone, s2.at[k]).wait()
        halo(k, True).wait_send()
        halo(k, False).wait_send()
        if k < SLOTS_DEV - 1:
            pltpu.make_async_copy(stage.at[k], stage.at[k], s3.at[k]).wait()
            across(k, 1).wait_send()

            @pl.when(xl != owner(k))
            def _():
                across(k, 0).wait_send()
        else:
            gone = parts.at[k, pl.ds(0, 448), :]
            pltpu.make_async_copy(gone, gone, s4.at[0]).wait()

            @pl.when(xl != owner(k))
            def _():
                direct(0).wait_send()


def per_device(psi_sectors, stiff_blocks, mass_blocks, harmonic_table):
    anywhere = pl.BlockSpec(memory_space=pl.ANY)
    vmem = pl.BlockSpec(memory_space=pltpu.VMEM)
    bf16, f32 = jnp.bfloat16, jnp.float32
    dma = pltpu.SemaphoreType.DMA
    return pl.pallas_call(
        kernel,
        out_shape=(
            jax.ShapeDtypeStruct((2, 64, 512), f32),
            jax.ShapeDtypeStruct((2, 64, 512), f32),
        ),
        in_specs=[anywhere, anywhere, anywhere, pl.BlockSpec(memory_space=pltpu.SMEM)],
        out_specs=(vmem, vmem),
        scratch_shapes=[
            pltpu.VMEM((NCHUNK, 64, PIECE, M), bf16),
            pltpu.VMEM((NCHUNK, 64, PIECE, M), bf16),
            pltpu.VMEM((SLOTS_DEV, 2, SEG + 2 * HALO, M), bf16),
            pltpu.VMEM((2, 1024, 1024), bf16),
            pltpu.VMEM((8, 2 * B, NBAND * B), bf16),
            pltpu.VMEM((CHUNK, 4 * M), bf16),
            pltpu.VMEM((2 * M, 4 * M), f32),
            pltpu.VMEM((SLOTS_DEV, 2 * M, 4 * M), bf16),
            pltpu.VMEM((SLOTS_DEV - 1, 3, 128, 4 * M), bf16),
            pltpu.VMEM((SLOTS_DEV - 1, 128, 4 * M), bf16),
            pltpu.VMEM((2, 4, 64, 4 * M), bf16),
            pltpu.VMEM((16, 64, 4 * M), bf16),
            dma((2, NBAND)),
            dma((NCHUNK,)),
            dma((NCHUNK,)),
            dma((SLOTS_DEV,)),
            dma((SLOTS_DEV, NCHUNK)),
            dma((SLOTS_DEV, 2)),
            dma((SLOTS_DEV, 2)),
            dma((SLOTS_DEV - 1,)),
            dma((SLOTS_DEV - 1,)),
            dma((2,)),
            dma,
            dma((SLOTS_DEV - 1, 2)),
            dma((2,)),
        ],
        compiler_params=pltpu.CompilerParams(
            collective_id=0, has_side_effects=True, vmem_limit_bytes=60 * 1024 * 1024
        ),
        name="reduce_sectors",
    )(psi_sectors, stiff_blocks, mass_blocks, harmonic_table)


def solution(mesh):
    placed = (P("sector", "row", None), P("row", None, None, None), P("row", None, None, None), P())
    return jax.shard_map(
        per_device,
        mesh=mesh,
        in_specs=placed,
        out_specs=(P("sector", "row", None), P("sector", "row", None)),
        check_vma=False,
    )
```

```python
import functools
import math

import jax
import jax.numpy as jnp
from jax import lax
from jax.experimental import pallas as pl
from jax.experimental.pallas import tpu as pltpu
from jax.sharding import PartitionSpec as P

MESH = pl.DeviceIdType.MESH
B = 128
M = 256
NBAND = 5
ROWS_DEV = 2048
SEG = 1024
CHUNK = 256
NCHUNK = 4
PIECE = 32
TILE = 16
SLOTS_DEV = 4
ORDER = (3, 0, 1, 2)
HALO = 256
WIDE = 512
SECTORS = 64
SLOTS = 32
SECTOR_OFFSETS = tuple(
    (dy, dx, dc) for dy in (2, 1, 3, 0) for dx in (1, 0) for dc in (0, 1) if dy or dx or dc
)
OWNER_OFFSETS = tuple((dy, dc) for dy in (2, 1, 3, 0) for dc in (0, 1) if dy or dc)


def coefficients(table):
    shape = (2 * SLOTS, SECTORS)
    line = lax.broadcasted_iota(jnp.int32, shape, 0)
    sector = lax.broadcasted_iota(jnp.int32, shape, 1)
    pair = jnp.zeros(shape, jnp.int32)
    for j in range(SLOTS):
        pair = jnp.where(line % SLOTS == j, table[j], pair)
    first = line < SLOTS
    zero = pair == 0
    freq = jnp.where(jnp.logical_and(zero, jnp.logical_not(first)), SECTORS // 2, pair)
    shift = jnp.where(jnp.logical_or(first, zero), 0, 3 * SECTORS // 4)
    phase = (freq * sector + shift) % SECTORS
    wave = jnp.cos(phase.astype(jnp.float32) * (2.0 * math.pi / SECTORS))
    return jnp.where(zero, math.sqrt(1.0 / SECTORS), math.sqrt(2.0 / SECTORS)) * wave


def kernel(
    psi, stiff, mass, table, out_k, out_m,
    arrived, sent, fields, lift, bands, images, total, parts,
    stiff_in, stiff_mid, stiff_end, mass_in, mass_mid, mass_end,
    load_sem, s1, r1, s2, r2, sh, rh, sk1, rk1, sk2, rk2, sm1, rm1, sm2, rm2,
):
    sec = lax.axis_index("sector")
    row = lax.axis_index("row")
    y, xl, core = sec // 4, (sec // 2) % 2, sec % 2
    turn = y * 2 + core
    seg = row * 2 + xl
    z, xh = row // 2, row % 2

    def device(y_, xl_, core_, row_):
        return {"sector": y_ * 4 + xl_ * 2 + core_, "row": row_}

    loads = []
    for m, src in enumerate((stiff, mass)):
        for k in range(NBAND):
            copy = pltpu.make_async_copy(
                src.at[pl.ds(pl.multiple_of(xl * 8, 8), 8), k],
                bands.at[:, pl.ds(m * B, B), pl.ds(k * B, B)],
                load_sem.at[m, k],
            )
            copy.start()
            loads.append(copy)

    barrier = pltpu.get_barrier_semaphore()
    count = 0
    for dy, dx, dc in SECTOR_OFFSETS:
        pl.semaphore_signal(
            barrier, inc=1, device_id_type=MESH,
            device_id=device((y + dy) % 4, (xl + dx) % 2, (core + dc) % 2, row),
        )
        count += 1
    for dr in range(1, 8):
        for dx in range(2):
            pl.semaphore_signal(
                barrier, inc=1, device_id_type=MESH,
                device_id=device(y, (xl + dx) % 2, core, (row + dr) % 8),
            )
            count += 1
    with jax.named_scope("barrier"):
        pl.semaphore_wait(barrier, count)

    def rows_of(xl_, turn_, q):
        return pl.ds(pl.multiple_of(xl_ * SEG + q * CHUNK + turn_ * PIECE, PIECE), PIECE)

    for q in ORDER:
        for dy, dx, dc in SECTOR_OFFSETS:
            y_, xl_, core_ = (y + dy) % 4, (xl + dx) % 2, (core + dc) % 2
            pltpu.make_async_remote_copy(
                src_ref=psi.at[:, rows_of(xl_, y_ * 2 + core_, q), :],
                dst_ref=arrived.at[q, pl.ds(sec * 4, 4)],
                send_sem=s1.at[q],
                recv_sem=r1.at[q],
                device_id=device(y_, xl_, core_, row),
                device_id_type=MESH,
            ).start()
        pltpu.make_async_copy(
            psi.at[:, rows_of(xl, turn, q), :], arrived.at[q, pl.ds(sec * 4, 4)], r1.at[q]
        ).start()

    coef = coefficients(table)
    coef_hi = coef.astype(jnp.bfloat16)
    coef_lo = (coef - coef_hi.astype(jnp.float32)).astype(jnp.bfloat16)
    quarter = 256

    def spread(n, _):
        i = lax.broadcasted_iota(jnp.int32, (quarter, 64), 0) + n * quarter
        g = i // TILE
        e, t, k = g % 2, (g // 2) % 8, g // 16
        slot = (t // 2) * 8 + ((k // 2 + t) % 2) * 4 + (t % 2) * 2 + k % 2
        want = e * 32 + slot
        pick = (lax.broadcasted_iota(jnp.int32, (quarter, 64), 1) == want).astype(jnp.bfloat16)
        col = lax.broadcasted_iota(jnp.int32, (64, 1024), 1) // TILE
        wide = (lax.broadcasted_iota(jnp.int32, (64, 1024), 0) == col).astype(jnp.bfloat16)
        same = (
            lax.broadcasted_iota(jnp.int32, (quarter, 1024), 0) % TILE
            == lax.broadcasted_iota(jnp.int32, (quarter, 1024), 1) % TILE
        )
        for h, part in enumerate((coef_hi, coef_lo)):
            chosen = jnp.dot(pick, part, preferred_element_type=jnp.float32).astype(jnp.bfloat16)
            full = jnp.dot(chosen, wide, preferred_element_type=jnp.float32)
            lift[h, pl.ds(pl.multiple_of(n * quarter, quarter), quarter), :] = jnp.where(
                same, full, 0.0
            ).astype(jnp.bfloat16)
        return 0

    with jax.named_scope("spread"):
        lax.fori_loop(0, 4, spread, 0)

    def send_fields(k, q):
        mine = pl.ds(pl.multiple_of(HALO + q * CHUNK + turn * PIECE, PIECE), PIECE)
        for dy, dc in OWNER_OFFSETS:
            y_, core_ = (y + dy) % 4, (core + dc) % 2
            pltpu.make_async_remote_copy(
                src_ref=sent.at[q, pl.ds(k * 16 + (y_ * 2 + core_) * 2, 2)],
                dst_ref=fields.at[k, :, mine, :],
                send_sem=s2.at[k],
                recv_sem=r2.at[k, q],
                device_id=device(y_, xl, core_, row),
                device_id_type=MESH,
            ).start()
        pltpu.make_async_copy(
            sent.at[q, pl.ds(k * 16 + turn * 2, 2)], fields.at[k, :, mine, :], r2.at[k, q]
        ).start()

    for q in ORDER:
        with jax.named_scope(f"wait_one#q={q}"):
            pltpu.make_async_copy(arrived.at[q], arrived.at[q], r1.at[q]).wait()

        def transform(h, _):
            rows = pl.ds(pl.multiple_of(h * TILE, TILE), TILE)
            x = arrived[q, :, rows, :].reshape(64 * TILE, M)
            for n in range(2):
                at = pl.ds(n * 512, 512)
                out = jnp.dot(lift[0, at, :], x, preferred_element_type=jnp.float32)
                out += jnp.dot(lift[1, at, :], x, preferred_element_type=jnp.float32)
                sent[q, pl.ds(n * 32, 32), rows, :] = out.astype(jnp.bfloat16).reshape(
                    32, TILE, M
                )
            return 0

        with jax.named_scope(f"transform#q={q}"):
            lax.fori_loop(0, PIECE // TILE, transform, 0)
        for k in (0, 1) if q in (3, 0) else (0,):
            send_fields(k, q)
    for k, q in ((2, 3), (2, 0), (1, 1), (1, 2)):
        send_fields(k, q)

    for copy in loads:
        copy.wait()

    def process(k, q, first):
        for b in range(2):
            i = 2 * q + b
            for e in range(2):
                window = fields[k, e, pl.ds(i * B, NBAND * B), :]
                w = jnp.dot(bands[i], window, preferred_element_type=jnp.float32)
                w = w.astype(jnp.bfloat16)
                images[pl.ds(b * B, B), pl.ds(e * M, M)] = w[:B]
                images[pl.ds(b * B, B), pl.ds(2 * M + e * M, M)] = w[B:]
        for e in range(2):
            left = fields[k, e, pl.ds(HALO + q * CHUNK, CHUNK), :]
            part = lax.dot_general(
                left, images[...], (((0,), (0,)), ((), ())), preferred_element_type=jnp.float32
            )
            at = pl.ds(e * M, M)
            if first:
                total[at, :] = part
            else:
                total[at, :] += part

    def arrival(k, q):
        whole = fields.at[k, :, pl.ds(0, CHUNK), :]
        with jax.named_scope(f"wait_two#k={k}#q={q}"):
            pltpu.make_async_copy(whole, whole, r2.at[k, q]).wait()

    def halo(k, up):
        to = (seg + (1 if up else 15)) % 16
        src, dst = (SEG, 0) if up else (HALO, HALO + SEG)
        side = 0 if up else 1
        return pltpu.make_async_remote_copy(
            src_ref=fields.at[k, :, pl.ds(src, HALO), :],
            dst_ref=fields.at[k, :, pl.ds(dst, HALO), :],
            send_sem=sh.at[k, side],
            recv_sem=rh.at[k, side],
            device_id=device(y, to % 2, core, to // 2),
            device_id_type=MESH,
        )

    def margins(k):
        arrival(k, 3)
        halo(k, True).start()
        arrival(k, 0)
        halo(k, False).start()

    def slot(k):
        arrival(k, 1)
        with jax.named_scope(f"wait_low#k={k}"):
            halo(k, True).wait_recv()
        with jax.named_scope(f"process#k={k}#q=0"):
            process(k, 0, True)
        arrival(k, 2)
        with jax.named_scope(f"process#k={k}#q=1"):
            process(k, 1, False)
        with jax.named_scope(f"process#k={k}#q=2"):
            process(k, 2, False)
        with jax.named_scope(f"wait_high#k={k}"):
            halo(k, False).wait_recv()
        with jax.named_scope(f"process#k={k}#q=3"):
            process(k, 3, False)
        with jax.named_scope(f"narrow#k={k}"):
            parts[k] = total[...].astype(jnp.bfloat16).reshape(4, 2, 64, 2 * WIDE)
        for dz in (2, 1, 3):
            stiff_first(k, dz).start()
        mass_first(k, 1).start()

        @pl.when(xl == owner(k))
        def _():
            pltpu.make_async_copy(
                parts.at[k, :, xh, :, pl.ds(WIDE, WIDE)], mass_in.at[k % 2, place], rm1.at[k % 2]
            ).start()

        @pl.when(xl != owner(k))
        def _():
            mass_first(k, 0).start()

    place = xh * 2 + xl

    def owner(k):
        return (k // 2 + core) % 2

    def stiff_first(k, dz):
        z_ = (z + dz) % 4
        return pltpu.make_async_remote_copy(
            src_ref=parts.at[k, z_, :, :, pl.ds(0, WIDE)],
            dst_ref=stiff_in.at[k, 3 - dz],
            send_sem=sk1.at[k],
            recv_sem=rk1.at[k],
            device_id=device(y, xl, core, z_ * 2 + xh),
            device_id_type=MESH,
        )

    def stiff_second(k, dh):
        xh_ = (xh + dh) % 2
        return pltpu.make_async_remote_copy(
            src_ref=stiff_mid.at[k, xh_],
            dst_ref=stiff_end.at[k % 2, place],
            send_sem=sk2.at[k, dh],
            recv_sem=rk2.at[k % 2],
            device_id=device(y, owner(k), core, z * 2 + xh_),
            device_id_type=MESH,
        )

    def mass_first(k, dh):
        xh_ = (xh + dh) % 2
        return pltpu.make_async_remote_copy(
            src_ref=parts.at[k, :, xh_, :, pl.ds(WIDE, WIDE)],
            dst_ref=mass_in.at[k % 2, place],
            send_sem=sm1.at[k, dh],
            recv_sem=rm1.at[k % 2],
            device_id=device(y, owner(k), core, z * 2 + xh_),
            device_id_type=MESH,
        )

    def mass_second(k, dz):
        z_ = (z + dz) % 4
        return pltpu.make_async_remote_copy(
            src_ref=mass_mid.at[k % 2, z_],
            dst_ref=mass_end.at[k % 2, 3 - dz],
            send_sem=sm2.at[k % 2],
            recv_sem=rm2.at[k % 2],
            device_id=device(y, xl, core, z_ * 2 + xh),
            device_id_type=MESH,
        )

    def whole(ref, sem):
        pltpu.make_async_copy(ref, ref, sem).wait()

    def second(k):
        with jax.named_scope(f"wait_stiff#k={k}"):
            whole(stiff_in.at[k], rk1.at[k])
        acc = parts[k, z, :, :, pl.ds(0, WIDE)].astype(jnp.float32)
        for n in range(3):
            acc += stiff_in[k, n].astype(jnp.float32)
        stiff_mid[k] = acc.astype(jnp.bfloat16)
        stiff_second(k, 1).start()

        @pl.when(xl == owner(k))
        def _():
            pltpu.make_async_copy(
                stiff_mid.at[k, xh], stiff_end.at[k % 2, place], rk2.at[k % 2]
            ).start()
            with jax.named_scope(f"wait_mass#k={k}"):
                whole(mass_in.at[k % 2], rm1.at[k % 2])
            acc = mass_in[k % 2, 0].astype(jnp.float32)
            for n in range(1, 4):
                acc += mass_in[k % 2, n].astype(jnp.float32)
            mass_mid[k % 2] = acc.astype(jnp.bfloat16)
            for dz in (2, 1, 3):
                mass_second(k, dz).start()

        @pl.when(xl != owner(k))
        def _():
            stiff_second(k, 0).start()

    margins(0)
    margins(1)
    slot(0)
    for k, q in ((3, 3), (3, 0), (2, 1), (2, 2)):
        send_fields(k, q)
    margins(2)
    slot(1)
    for q in (1, 2):
        send_fields(3, q)
    second(0)
    margins(3)
    slot(2)
    second(1)
    slot(3)
    second(2)
    second(3)

    for k in range(2):
        with jax.named_scope(f"wait_end#k={k}"):
            whole(stiff_end.at[k], rk2.at[k])
            whole(mass_end.at[k], rm2.at[k])
        acc = stiff_end[k, 0].astype(jnp.float32)
        for n in range(1, 4):
            acc += stiff_end[k, n].astype(jnp.float32)
        out_k[k] = acc
        acc = mass_mid[k, z].astype(jnp.float32)
        for n in range(3):
            acc += mass_end[k, n].astype(jnp.float32)
        out_m[k] = acc

    for q in range(NCHUNK):
        gone = arrived.at[q, pl.ds(0, 60)]
        pltpu.make_async_copy(gone, gone, s1.at[q]).wait()
    for k in range(SLOTS_DEV):
        gone = sent.at[pl.ds(0, 4), pl.ds(0, 14)]
        pltpu.make_async_copy(gone, gone, s2.at[k]).wait()
        halo(k, True).wait_send()
        halo(k, False).wait_send()
        whole(stiff_in.at[k], sk1.at[k])
        stiff_second(k, 1).wait_send()
        mass_first(k, 1).wait_send()

        @pl.when(xl != owner(k))
        def _():
            stiff_second(k, 0).wait_send()
            mass_first(k, 0).wait_send()

    for k in range(2):
        whole(mass_end.at[k], sm2.at[k])


def per_device(psi_sectors, stiff_blocks, mass_blocks, harmonic_table):
    anywhere = pl.BlockSpec(memory_space=pl.ANY)
    vmem = pl.BlockSpec(memory_space=pltpu.VMEM)
    bf16, f32 = jnp.bfloat16, jnp.float32
    dma = pltpu.SemaphoreType.DMA
    return pl.pallas_call(
        kernel,
        out_shape=(
            jax.ShapeDtypeStruct((2, 64, 512), f32),
            jax.ShapeDtypeStruct((2, 64, 512), f32),
        ),
        in_specs=[anywhere, anywhere, anywhere, pl.BlockSpec(memory_space=pltpu.SMEM)],
        out_specs=(vmem, vmem),
        scratch_shapes=[
            pltpu.VMEM((NCHUNK, 64, PIECE, M), bf16),
            pltpu.VMEM((NCHUNK, 64, PIECE, M), bf16),
            pltpu.VMEM((SLOTS_DEV, 2, SEG + 2 * HALO, M), bf16),
            pltpu.VMEM((2, 1024, 1024), bf16),
            pltpu.VMEM((8, 2 * B, NBAND * B), bf16),
            pltpu.VMEM((CHUNK, 4 * M), bf16),
            pltpu.VMEM((2 * M, 4 * M), f32),
            pltpu.VMEM((SLOTS_DEV, 4, 2, 64, 2 * WIDE), bf16),
            pltpu.VMEM((SLOTS_DEV, 3, 2, 64, WIDE), bf16),
            pltpu.VMEM((SLOTS_DEV, 2, 64, WIDE), bf16),
            pltpu.VMEM((2, 4, 64, WIDE), bf16),
            pltpu.VMEM((2, 4, 4, 64, WIDE), bf16),
            pltpu.VMEM((2, 4, 64, WIDE), bf16),
            pltpu.VMEM((2, 3, 64, WIDE), bf16),
            dma((2, NBAND)),
            dma((NCHUNK,)),
            dma((NCHUNK,)),
            dma((SLOTS_DEV,)),
            dma((SLOTS_DEV, NCHUNK)),
            dma((SLOTS_DEV, 2)),
            dma((SLOTS_DEV, 2)),
            dma((SLOTS_DEV,)),
            dma((SLOTS_DEV,)),
            dma((SLOTS_DEV, 2)),
            dma((2,)),
            dma((SLOTS_DEV, 2)),
            dma((2,)),
            dma((2,)),
            dma((2,)),
        ],
        compiler_params=pltpu.CompilerParams(
            collective_id=0, has_side_effects=True, vmem_limit_bytes=60 * 1024 * 1024
        ),
        name="reduce_sectors",
    )(psi_sectors, stiff_blocks, mass_blocks, harmonic_table)


def solution(mesh):
    placed = (P("sector", "row", None), P("row", None, None, None), P("row", None, None, None), P())
    return jax.shard_map(
        per_device,
        mesh=mesh,
        in_specs=placed,
        out_specs=(P("sector", "row", None), P("sector", "row", None)),
        check_vma=False,
    )
```

```python
import functools
import math

import jax
import jax.numpy as jnp
from jax import lax
from jax.experimental import pallas as pl
from jax.experimental.pallas import tpu as pltpu
from jax.sharding import PartitionSpec as P

MESH = pl.DeviceIdType.MESH
B = 128
M = 256
NBAND = 5
ROWS_DEV = 2048
SEG = 1024
CHUNK = 256
NCHUNK = 4
PIECE = 32
TILE = 16
SLOTS_DEV = 4
ORDER = (3, 0, 1, 2)
HALO = 256
WIDE = 512
SECTORS = 64
SLOTS = 32
SECTOR_OFFSETS = tuple(
    (dy, dx, dc) for dy in (2, 1, 3, 0) for dx in (1, 0) for dc in (0, 1) if dy or dx or dc
)
OWNER_OFFSETS = tuple((dy, dc) for dy in (2, 1, 3, 0) for dc in (0, 1) if dy or dc)


def coefficients(table):
    shape = (2 * SLOTS, SECTORS)
    line = lax.broadcasted_iota(jnp.int32, shape, 0)
    sector = lax.broadcasted_iota(jnp.int32, shape, 1)
    pair = jnp.zeros(shape, jnp.int32)
    for j in range(SLOTS):
        pair = jnp.where(line % SLOTS == j, table[j], pair)
    first = line < SLOTS
    zero = pair == 0
    freq = jnp.where(jnp.logical_and(zero, jnp.logical_not(first)), SECTORS // 2, pair)
    shift = jnp.where(jnp.logical_or(first, zero), 0, 3 * SECTORS // 4)
    phase = (freq * sector + shift) % SECTORS
    wave = jnp.cos(phase.astype(jnp.float32) * (2.0 * math.pi / SECTORS))
    return jnp.where(zero, math.sqrt(1.0 / SECTORS), math.sqrt(2.0 / SECTORS)) * wave


def kernel(
    psi, stiff, mass, table, out,
    arrived, sent, fields, lift, bands, edges, images, total, parts,
    stiff_in, stiff_mid, stiff_end, mass_in, mass_mid, mass_end, result, done,
    load_sem, s1, r1, s2, r2, sh, rh, sk1, rk1, sk2, rk2, sm1, rm1, sm2, rm2,
):
    sec = lax.axis_index("sector")
    row = lax.axis_index("row")
    y, xl, core = sec // 4, (sec // 2) % 2, sec % 2
    turn = y * 2 + core
    seg = row * 2 + xl
    z, xh = row // 2, row % 2

    def device(y_, xl_, core_, row_):
        return {"sector": y_ * 4 + xl_ * 2 + core_, "row": row_}

    loads = []
    for m, src in enumerate((stiff, mass)):
        for k in range(NBAND):
            copy = pltpu.make_async_copy(
                src.at[pl.ds(pl.multiple_of(xl * 8, 8), 8), k],
                bands.at[:, pl.ds(m * B, B), pl.ds(k * B, B)],
                load_sem.at[m, k],
            )
            copy.start()
            loads.append(copy)

    barrier = pltpu.get_barrier_semaphore()
    count = 0
    for dy, dx, dc in SECTOR_OFFSETS:
        pl.semaphore_signal(
            barrier, inc=1, device_id_type=MESH,
            device_id=device((y + dy) % 4, (xl + dx) % 2, (core + dc) % 2, row),
        )
        count += 1
    for dr in range(1, 8):
        for dx in range(2):
            pl.semaphore_signal(
                barrier, inc=1, device_id_type=MESH,
                device_id=device(y, (xl + dx) % 2, core, (row + dr) % 8),
            )
            count += 1
    with jax.named_scope("barrier"):
        pl.semaphore_wait(barrier, count)

    def rows_of(xl_, turn_, q):
        return pl.ds(pl.multiple_of(xl_ * SEG + q * CHUNK + turn_ * PIECE, PIECE), PIECE)

    for q in ORDER:
        for dy, dx, dc in SECTOR_OFFSETS:
            y_, xl_, core_ = (y + dy) % 4, (xl + dx) % 2, (core + dc) % 2
            pltpu.make_async_remote_copy(
                src_ref=psi.at[:, rows_of(xl_, y_ * 2 + core_, q), :],
                dst_ref=arrived.at[q, pl.ds(sec * 4, 4)],
                send_sem=s1.at[q],
                recv_sem=r1.at[q],
                device_id=device(y_, xl_, core_, row),
                device_id_type=MESH,
            ).start()
        pltpu.make_async_copy(
            psi.at[:, rows_of(xl, turn, q), :], arrived.at[q, pl.ds(sec * 4, 4)], r1.at[q]
        ).start()

    coef = coefficients(table)
    coef_hi = coef.astype(jnp.bfloat16)
    coef_lo = (coef - coef_hi.astype(jnp.float32)).astype(jnp.bfloat16)
    quarter = 256

    def spread(n, _):
        i = lax.broadcasted_iota(jnp.int32, (quarter, 64), 0) + n * quarter
        g = i // TILE
        e, t, k = g % 2, (g // 2) % 8, g // 16
        slot = (t // 2) * 8 + ((k // 2 + t) % 2) * 4 + (t % 2) * 2 + k % 2
        want = e * 32 + slot
        pick = (lax.broadcasted_iota(jnp.int32, (quarter, 64), 1) == want).astype(jnp.bfloat16)
        col = lax.broadcasted_iota(jnp.int32, (64, 1024), 1) // TILE
        wide = (lax.broadcasted_iota(jnp.int32, (64, 1024), 0) == col).astype(jnp.bfloat16)
        same = (
            lax.broadcasted_iota(jnp.int32, (quarter, 1024), 0) % TILE
            == lax.broadcasted_iota(jnp.int32, (quarter, 1024), 1) % TILE
        )
        for h, part in enumerate((coef_hi, coef_lo)):
            chosen = jnp.dot(pick, part, preferred_element_type=jnp.float32).astype(jnp.bfloat16)
            full = jnp.dot(chosen, wide, preferred_element_type=jnp.float32)
            lift[h, pl.ds(pl.multiple_of(n * quarter, quarter), quarter), :] = jnp.where(
                same, full, 0.0
            ).astype(jnp.bfloat16)
        return 0

    with jax.named_scope("spread"):
        lax.fori_loop(0, 4, spread, 0)

    def send_fields(k, q):
        mine = pl.ds(pl.multiple_of(HALO + q * CHUNK + turn * PIECE, PIECE), PIECE)
        for dy, dc in OWNER_OFFSETS:
            y_, core_ = (y + dy) % 4, (core + dc) % 2
            pltpu.make_async_remote_copy(
                src_ref=sent.at[q, pl.ds(k * 16 + (y_ * 2 + core_) * 2, 2)],
                dst_ref=fields.at[k, :, mine, :],
                send_sem=s2.at[k],
                recv_sem=r2.at[k, q],
                device_id=device(y_, xl, core_, row),
                device_id_type=MESH,
            ).start()
        pltpu.make_async_copy(
            sent.at[q, pl.ds(k * 16 + turn * 2, 2)], fields.at[k, :, mine, :], r2.at[k, q]
        ).start()

    for q in ORDER:
        with jax.named_scope(f"wait_one#q={q}"):
            pltpu.make_async_copy(arrived.at[q], arrived.at[q], r1.at[q]).wait()

        def transform(h, _):
            rows = pl.ds(pl.multiple_of(h * TILE, TILE), TILE)
            x = arrived[q, :, rows, :].reshape(64 * TILE, M)
            for n in range(2):
                at = pl.ds(n * 512, 512)
                out = jnp.dot(lift[0, at, :], x, preferred_element_type=jnp.float32)
                out += jnp.dot(lift[1, at, :], x, preferred_element_type=jnp.float32)
                sent[q, pl.ds(n * 32, 32), rows, :] = out.astype(jnp.bfloat16).reshape(
                    32, TILE, M
                )
            return 0

        with jax.named_scope(f"transform#q={q}"):
            lax.fori_loop(0, PIECE // TILE, transform, 0)
        for k in (0, 1) if q in (3, 0) else (0,):
            send_fields(k, q)
    for k, q in ((2, 3), (2, 0), (1, 1), (1, 2)):
        send_fields(k, q)

    for copy in loads:
        copy.wait()

    blank = pl.ds(pl.multiple_of((1 - core) * (HALO + SEG), HALO), HALO)
    for k in range(SLOTS_DEV):
        fields[k, :, blank, :] = jnp.zeros((2, HALO, M), jnp.bfloat16)
    near_block, far_block = core * 7, 1 + core * 5
    for n, (block, lane) in enumerate(
        ((near_block, B + core * 2 * B), (far_block, core * 4 * B), (near_block, core * 4 * B))
    ):
        for m in range(2):
            piece = bands[block, pl.ds(m * B, B), pl.ds(pl.multiple_of(lane, B), B)]
            edges[n, pl.ds(m * B, B), :] = piece.astype(jnp.float32).T.astype(jnp.bfloat16)

    def project(rows, first):
        for e in range(2):
            part = lax.dot_general(
                rows[e], images[...], (((0,), (0,)), ((), ())), preferred_element_type=jnp.float32
            )
            at = pl.ds(e * M, M)
            if first:
                total[at, :] = part
            else:
                total[at, :] += part

    def process(k, q):
        for b in range(2):
            i = 2 * q + b
            for e in range(2):
                window = fields[k, e, pl.ds(i * B, NBAND * B), :]
                w = jnp.dot(bands[i], window, preferred_element_type=jnp.float32)
                w = w.astype(jnp.bfloat16)
                images[pl.ds(b * B, B), pl.ds(e * M, M)] = w[:B]
                images[pl.ds(b * B, B), pl.ds(2 * M + e * M, M)] = w[B:]
        project(fields.at[k, :, pl.ds(HALO + q * CHUNK, CHUNK), :], False)

    def arrival(k, q):
        whole = fields.at[k, :, pl.ds(0, CHUNK), :]
        with jax.named_scope(f"wait_two#k={k}#q={q}"):
            pltpu.make_async_copy(whole, whole, r2.at[k, q]).wait()

    edge_rows = pl.ds(pl.multiple_of(core * (HALO + SEG), HALO), HALO)

    def halo(k):
        to = (seg + 1 + 14 * core) % 16
        mine = pl.ds(pl.multiple_of(SEG - core * (SEG - HALO), HALO), HALO)
        return pltpu.make_async_remote_copy(
            src_ref=fields.at[k, :, mine, :],
            dst_ref=fields.at[k, :, edge_rows, :],
            send_sem=sh.at[k],
            recv_sem=rh.at[k],
            device_id=device(y, to % 2, core, to // 2),
            device_id_type=MESH,
        )

    def margins(k):
        arrival(k, 3)

        @pl.when(core == 0)
        def _():
            halo(k).start()

        arrival(k, 0)

        @pl.when(core == 1)
        def _():
            halo(k).start()

    def boundary(k):
        near = pl.ds(pl.multiple_of(HALO + core * 7 * B, B), B)
        far = pl.ds(pl.multiple_of(HALO + B + core * 5 * B, B), B)
        for e in range(2):
            low = jnp.dot(edges[0], fields[k, e, near, :], preferred_element_type=jnp.float32)
            low += jnp.dot(edges[1], fields[k, e, far, :], preferred_element_type=jnp.float32)
            deep = jnp.dot(edges[2], fields[k, e, near, :], preferred_element_type=jnp.float32)
            low, deep = low.astype(jnp.bfloat16), deep.astype(jnp.bfloat16)
            at_low = pl.ds(pl.multiple_of((1 - core) * B, B), B)
            at_deep = pl.ds(pl.multiple_of(core * B, B), B)
            for m in range(2):
                columns = pl.ds(m * 2 * M + e * M, M)
                images[at_low, columns] = low[m * B : (m + 1) * B]
                images[at_deep, columns] = deep[m * B : (m + 1) * B]
        project(fields.at[k, :, edge_rows, :], True)

    def slot(k):
        with jax.named_scope(f"wait_halo#k={k}"):
            halo(k).wait_recv()
        with jax.named_scope(f"boundary#k={k}"):
            boundary(k)
        arrival(k, 1)
        with jax.named_scope(f"process#k={k}#q=0"):
            process(k, 0)
        arrival(k, 2)
        with jax.named_scope(f"process#k={k}#q=1"):
            process(k, 1)
        with jax.named_scope(f"process#k={k}#q=2"):
            process(k, 2)
        with jax.named_scope(f"process#k={k}#q=3"):
            process(k, 3)
        with jax.named_scope(f"narrow#k={k}"):
            parts[k] = total[...].astype(jnp.bfloat16).reshape(4, 2, 64, 2 * WIDE)
        for dz in (2, 1, 3):
            stiff_first(k, dz).start()
        mass_first(k, 1).start()

        @pl.when(xl == owner(k))
        def _():
            pltpu.make_async_copy(
                parts.at[k, :, xh, :, pl.ds(WIDE, WIDE)], mass_in.at[k % 2, place], rm1.at[k % 2]
            ).start()

        @pl.when(xl != owner(k))
        def _():
            mass_first(k, 0).start()

    place = xh * 2 + xl

    def owner(k):
        return (k // 2 + core) % 2

    def stiff_first(k, dz):
        z_ = (z + dz) % 4
        return pltpu.make_async_remote_copy(
            src_ref=parts.at[k, z_, :, :, pl.ds(0, WIDE)],
            dst_ref=stiff_in.at[k, 3 - dz],
            send_sem=sk1.at[k],
            recv_sem=rk1.at[k],
            device_id=device(y, xl, core, z_ * 2 + xh),
            device_id_type=MESH,
        )

    def stiff_second(k, dh):
        xh_ = (xh + dh) % 2
        return pltpu.make_async_remote_copy(
            src_ref=stiff_mid.at[k, xh_],
            dst_ref=stiff_end.at[k % 2, place],
            send_sem=sk2.at[k, dh],
            recv_sem=rk2.at[k % 2],
            device_id=device(y, owner(k), core, z * 2 + xh_),
            device_id_type=MESH,
        )

    def mass_first(k, dh):
        xh_ = (xh + dh) % 2
        return pltpu.make_async_remote_copy(
            src_ref=parts.at[k, :, xh_, :, pl.ds(WIDE, WIDE)],
            dst_ref=mass_in.at[k % 2, place],
            send_sem=sm1.at[k, dh],
            recv_sem=rm1.at[k % 2],
            device_id=device(y, owner(k), core, z * 2 + xh_),
            device_id_type=MESH,
        )

    def mass_second(k, dz):
        z_ = (z + dz) % 4
        return pltpu.make_async_remote_copy(
            src_ref=mass_mid.at[k % 2, z_],
            dst_ref=mass_end.at[k % 2, 3 - dz],
            send_sem=sm2.at[k % 2],
            recv_sem=rm2.at[k % 2],
            device_id=device(y, xl, core, z_ * 2 + xh),
            device_id_type=MESH,
        )

    def whole(ref, sem):
        pltpu.make_async_copy(ref, ref, sem).wait()

    def second(k):
        with jax.named_scope(f"wait_stiff#k={k}"):
            whole(stiff_in.at[k], rk1.at[k])
        acc = parts[k, z, :, :, pl.ds(0, WIDE)].astype(jnp.float32)
        for n in range(3):
            acc += stiff_in[k, n].astype(jnp.float32)
        stiff_mid[k] = acc.astype(jnp.bfloat16)
        stiff_second(k, 1).start()

        @pl.when(xl == owner(k))
        def _():
            pltpu.make_async_copy(
                stiff_mid.at[k, xh], stiff_end.at[k % 2, place], rk2.at[k % 2]
            ).start()
            with jax.named_scope(f"wait_mass#k={k}"):
                whole(mass_in.at[k % 2], rm1.at[k % 2])
            acc = mass_in[k % 2, 0].astype(jnp.float32)
            for n in range(1, 4):
                acc += mass_in[k % 2, n].astype(jnp.float32)
            mass_mid[k % 2] = acc.astype(jnp.bfloat16)
            for dz in (2, 1, 3):
                mass_second(k, dz).start()

        @pl.when(xl != owner(k))
        def _():
            stiff_second(k, 0).start()

    margins(0)
    margins(1)
    slot(0)
    for k, q in ((3, 3), (3, 0), (2, 1), (2, 2)):
        send_fields(k, q)
    margins(2)
    slot(1)
    for q in (1, 2):
        send_fields(3, q)
    second(0)
    margins(3)
    slot(2)
    slot(3)
    second(1)
    second(2)
    second(3)

    for k in range(2):
        with jax.named_scope(f"wait_end#k={k}"):
            whole(stiff_end.at[k], rk2.at[k])
            whole(mass_end.at[k], rm2.at[k])
        acc = stiff_end[k, 0].astype(jnp.float32)
        for n in range(1, 4):
            acc += stiff_end[k, n].astype(jnp.float32)
        result[0, k] = acc
        acc = mass_mid[k, z].astype(jnp.float32)
        for n in range(3):
            acc += mass_end[k, n].astype(jnp.float32)
        result[1, k] = acc

    final = pltpu.make_async_copy(result, out, done)
    final.start()
    for q in range(NCHUNK):
        gone = arrived.at[q, pl.ds(0, 60)]
        pltpu.make_async_copy(gone, gone, s1.at[q]).wait()
    for k in range(SLOTS_DEV):
        gone = sent.at[pl.ds(0, 4), pl.ds(0, 14)]
        pltpu.make_async_copy(gone, gone, s2.at[k]).wait()
        halo(k).wait_send()
        whole(stiff_in.at[k], sk1.at[k])
        stiff_second(k, 1).wait_send()
        mass_first(k, 1).wait_send()

        @pl.when(xl != owner(k))
        def _():
            stiff_second(k, 0).wait_send()
            mass_first(k, 0).wait_send()

    for k in range(2):
        whole(mass_end.at[k], sm2.at[k])
    final.wait()


def per_device(psi_sectors, stiff_blocks, mass_blocks, harmonic_table):
    anywhere = pl.BlockSpec(memory_space=pl.ANY)
    vmem = pl.BlockSpec(memory_space=pltpu.VMEM)
    bf16, f32 = jnp.bfloat16, jnp.float32
    dma = pltpu.SemaphoreType.DMA
    out = pl.pallas_call(
        kernel,
        out_shape=jax.ShapeDtypeStruct((2, 2, 64, 512), f32),
        in_specs=[anywhere, anywhere, anywhere, pl.BlockSpec(memory_space=pltpu.SMEM)],
        out_specs=pl.BlockSpec(memory_space=pl.ANY),
        scratch_shapes=[
            pltpu.VMEM((NCHUNK, 64, PIECE, M), bf16),
            pltpu.VMEM((NCHUNK, 64, PIECE, M), bf16),
            pltpu.VMEM((SLOTS_DEV, 2, SEG + 2 * HALO, M), bf16),
            pltpu.VMEM((2, 1024, 1024), bf16),
            pltpu.VMEM((8, 2 * B, NBAND * B), bf16),
            pltpu.VMEM((3, 2 * B, B), bf16),
            pltpu.VMEM((CHUNK, 4 * M), bf16),
            pltpu.VMEM((2 * M, 4 * M), f32),
            pltpu.VMEM((SLOTS_DEV, 4, 2, 64, 2 * WIDE), bf16),
            pltpu.VMEM((SLOTS_DEV, 3, 2, 64, WIDE), bf16),
            pltpu.VMEM((SLOTS_DEV, 2, 64, WIDE), bf16),
            pltpu.VMEM((2, 4, 64, WIDE), bf16),
            pltpu.VMEM((2, 4, 4, 64, WIDE), bf16),
            pltpu.VMEM((2, 4, 64, WIDE), bf16),
            pltpu.VMEM((2, 3, 64, WIDE), bf16),
            pltpu.VMEM((2, 2, 64, WIDE), f32),
            dma,
            dma((2, NBAND)),
            dma((NCHUNK,)),
            dma((NCHUNK,)),
            dma((SLOTS_DEV,)),
            dma((SLOTS_DEV, NCHUNK)),
            dma((SLOTS_DEV,)),
            dma((SLOTS_DEV,)),
            dma((SLOTS_DEV,)),
            dma((SLOTS_DEV,)),
            dma((SLOTS_DEV, 2)),
            dma((2,)),
            dma((SLOTS_DEV, 2)),
            dma((2,)),
            dma((2,)),
            dma((2,)),
        ],
        compiler_params=pltpu.CompilerParams(
            collective_id=0, has_side_effects=True, vmem_limit_bytes=52 * 1024 * 1024
        ),
        name="reduce_sectors",
    )(psi_sectors, stiff_blocks, mass_blocks, harmonic_table)
    return out[0], out[1]


def solution(mesh):
    placed = (P("sector", "row", None), P("row", None, None, None), P("row", None, None, None), P())
    return jax.shard_map(
        per_device,
        mesh=mesh,
        in_specs=placed,
        out_specs=(P("sector", "row", None), P("sector", "row", None)),
        check_vma=False,
    )
```

```python
import functools
import math

import jax
import jax.numpy as jnp
from jax import lax
from jax.experimental import pallas as pl
from jax.experimental.pallas import tpu as pltpu
from jax.sharding import PartitionSpec as P

MESH = pl.DeviceIdType.MESH
B = 128
M = 256
NBAND = 5
ROWS_DEV = 2048
SEG = 1024
CHUNK = 256
NCHUNK = 4
PIECE = 32
TILE = 16
SLOTS_DEV = 4
ORDER = (3, 0, 1, 2)
HALO = 256
WIDE = 512
SECTORS = 64
SLOTS = 32
SECTOR_OFFSETS = tuple(
    (dy, dx, dc) for dy in (2, 1, 3, 0) for dx in (1, 0) for dc in (0, 1) if dy or dx or dc
)
OWNER_OFFSETS = tuple((dy, dc) for dy in (2, 1, 3, 0) for dc in (0, 1) if dy or dc)


def coefficients(table):
    shape = (2 * SLOTS, SECTORS)
    line = lax.broadcasted_iota(jnp.int32, shape, 0)
    sector = lax.broadcasted_iota(jnp.int32, shape, 1)
    pair = jnp.zeros(shape, jnp.int32)
    for j in range(SLOTS):
        pair = jnp.where(line % SLOTS == j, table[j], pair)
    first = line < SLOTS
    zero = pair == 0
    freq = jnp.where(jnp.logical_and(zero, jnp.logical_not(first)), SECTORS // 2, pair)
    shift = jnp.where(jnp.logical_or(first, zero), 0, 3 * SECTORS // 4)
    phase = (freq * sector + shift) % SECTORS
    wave = jnp.cos(phase.astype(jnp.float32) * (2.0 * math.pi / SECTORS))
    return jnp.where(zero, math.sqrt(1.0 / SECTORS), math.sqrt(2.0 / SECTORS)) * wave


def kernel(
    psi, stiff, mass, table, out,
    arrived, sent, fields, lift, bands, edges, images, total, parts,
    stiff_in, stiff_mid, stiff_end, mass_in, mass_mid, mass_end, result, done,
    load_sem, s1, r1, s2, r2, sh, rh, sk1, rk1, sk2, rk2, sm1, rm1, sm2, rm2,
):
    sec = lax.axis_index("sector")
    row = lax.axis_index("row")
    y, xl, core = sec // 4, (sec // 2) % 2, sec % 2
    turn = y * 2 + core
    seg = row * 2 + xl
    z, xh = row // 2, row % 2

    def device(y_, xl_, core_, row_):
        return {"sector": y_ * 4 + xl_ * 2 + core_, "row": row_}

    loads = []
    for m, src in enumerate((stiff, mass)):
        for k in range(NBAND):
            copy = pltpu.make_async_copy(
                src.at[pl.ds(pl.multiple_of(xl * 8, 8), 8), k],
                bands.at[:, pl.ds(m * B, B), pl.ds(k * B, B)],
                load_sem.at[m, k],
            )
            copy.start()
            loads.append(copy)

    barrier = pltpu.get_barrier_semaphore()
    count = 0
    for dy, dx, dc in SECTOR_OFFSETS:
        pl.semaphore_signal(
            barrier, inc=1, device_id_type=MESH,
            device_id=device((y + dy) % 4, (xl + dx) % 2, (core + dc) % 2, row),
        )
        count += 1
    for dr in range(1, 8):
        for dx in range(2):
            pl.semaphore_signal(
                barrier, inc=1, device_id_type=MESH,
                device_id=device(y, (xl + dx) % 2, core, (row + dr) % 8),
            )
            count += 1
    with jax.named_scope("barrier"):
        pl.semaphore_wait(barrier, count)

    def rows_of(xl_, turn_, q):
        return pl.ds(pl.multiple_of(xl_ * SEG + q * CHUNK + turn_ * PIECE, PIECE), PIECE)

    for q in ORDER:
        for dy, dx, dc in SECTOR_OFFSETS:
            y_, xl_, core_ = (y + dy) % 4, (xl + dx) % 2, (core + dc) % 2
            pltpu.make_async_remote_copy(
                src_ref=psi.at[:, rows_of(xl_, y_ * 2 + core_, q), :],
                dst_ref=arrived.at[q, pl.ds(sec * 4, 4)],
                send_sem=s1.at[q],
                recv_sem=r1.at[q],
                device_id=device(y_, xl_, core_, row),
                device_id_type=MESH,
            ).start()
        pltpu.make_async_copy(
            psi.at[:, rows_of(xl, turn, q), :], arrived.at[q, pl.ds(sec * 4, 4)], r1.at[q]
        ).start()

    coef = coefficients(table)
    coef_hi = coef.astype(jnp.bfloat16)
    coef_lo = (coef - coef_hi.astype(jnp.float32)).astype(jnp.bfloat16)
    quarter = 256

    def spread(n, _):
        i = lax.broadcasted_iota(jnp.int32, (quarter, 64), 0) + n * quarter
        g = i // TILE
        e, t, k = g % 2, (g // 2) % 8, g // 16
        slot = (t // 2) * 8 + ((k // 2 + t) % 2) * 4 + (t % 2) * 2 + k % 2
        want = e * 32 + slot
        pick = (lax.broadcasted_iota(jnp.int32, (quarter, 64), 1) == want).astype(jnp.bfloat16)
        col = lax.broadcasted_iota(jnp.int32, (64, 1024), 1) // TILE
        wide = (lax.broadcasted_iota(jnp.int32, (64, 1024), 0) == col).astype(jnp.bfloat16)
        same = (
            lax.broadcasted_iota(jnp.int32, (quarter, 1024), 0) % TILE
            == lax.broadcasted_iota(jnp.int32, (quarter, 1024), 1) % TILE
        )
        for h, part in enumerate((coef_hi, coef_lo)):
            chosen = jnp.dot(pick, part, preferred_element_type=jnp.float32).astype(jnp.bfloat16)
            full = jnp.dot(chosen, wide, preferred_element_type=jnp.float32)
            lift[h, pl.ds(pl.multiple_of(n * quarter, quarter), quarter), :] = jnp.where(
                same, full, 0.0
            ).astype(jnp.bfloat16)
        return 0

    with jax.named_scope("spread"):
        lax.fori_loop(0, 4, spread, 0)

    def mine(q):
        return pl.ds(pl.multiple_of(HALO + q * CHUNK + turn * PIECE, PIECE), PIECE)

    def send_fields(k, chunk):
        for dy, dc in OWNER_OFFSETS:
            y_, core_ = (y + dy) % 4, (core + dc) % 2
            q = chunk(core_)
            pltpu.make_async_remote_copy(
                src_ref=sent.at[q, pl.ds(k * 16 + (y_ * 2 + core_) * 2, 2)],
                dst_ref=fields.at[k, :, mine(q), :],
                send_sem=s2.at[k],
                recv_sem=r2.at[k, q],
                device_id=device(y_, xl, core_, row),
                device_id_type=MESH,
            ).start()
        q = chunk(core)
        pltpu.make_async_copy(
            sent.at[q, pl.ds(k * 16 + turn * 2, 2)], fields.at[k, :, mine(q), :], r2.at[k, q]
        ).start()

    def first_chunk(core_):
        return 3 * (1 - core_)

    def second_chunk(core_):
        return 3 * core_

    def send_slot(k):
        send_fields(k, second_chunk)
        if k + 1 < SLOTS_DEV:
            send_fields(k + 1, first_chunk)
        send_fields(k, lambda core_: 1)
        send_fields(k, lambda core_: 2)

    for q in ORDER:
        with jax.named_scope(f"wait_one#q={q}"):
            pltpu.make_async_copy(arrived.at[q], arrived.at[q], r1.at[q]).wait()

        def transform(h, _):
            rows = pl.ds(pl.multiple_of(h * TILE, TILE), TILE)
            x = arrived[q, :, rows, :].reshape(64 * TILE, M)
            for n in range(2):
                at = pl.ds(n * 512, 512)
                out = jnp.dot(lift[0, at, :], x, preferred_element_type=jnp.float32)
                out += jnp.dot(lift[1, at, :], x, preferred_element_type=jnp.float32)
                sent[q, pl.ds(n * 32, 32), rows, :] = out.astype(jnp.bfloat16).reshape(
                    32, TILE, M
                )
            return 0

        with jax.named_scope(f"transform#q={q}"):
            lax.fori_loop(0, PIECE // TILE, transform, 0)
        send_fields(0, lambda core_: q)
        if q == 0:
            send_fields(1, first_chunk)
    send_slot(1)

    for copy in loads:
        copy.wait()

    blank = pl.ds(pl.multiple_of((1 - core) * (HALO + SEG), HALO), HALO)
    for k in range(SLOTS_DEV):
        fields[k, :, blank, :] = jnp.zeros((2, HALO, M), jnp.bfloat16)
    near_block, far_block = core * 7, 1 + core * 5
    for n, (block, lane) in enumerate(
        ((near_block, B + core * 2 * B), (far_block, core * 4 * B), (near_block, core * 4 * B))
    ):
        for m in range(2):
            piece = bands[block, pl.ds(m * B, B), pl.ds(pl.multiple_of(lane, B), B)]
            edges[n, pl.ds(m * B, B), :] = piece.astype(jnp.float32).T.astype(jnp.bfloat16)

    def project(rows, first):
        for e in range(2):
            part = lax.dot_general(
                rows[e], images[...], (((0,), (0,)), ((), ())), preferred_element_type=jnp.float32
            )
            at = pl.ds(e * M, M)
            if first:
                total[at, :] = part
            else:
                total[at, :] += part

    def process(k, q):
        for b in range(2):
            i = 2 * q + b
            for e in range(2):
                window = fields[k, e, pl.ds(i * B, NBAND * B), :]
                w = jnp.dot(bands[i], window, preferred_element_type=jnp.float32)
                w = w.astype(jnp.bfloat16)
                images[pl.ds(b * B, B), pl.ds(e * M, M)] = w[:B]
                images[pl.ds(b * B, B), pl.ds(2 * M + e * M, M)] = w[B:]
        project(fields.at[k, :, pl.ds(HALO + q * CHUNK, CHUNK), :], False)

    def arrival(k, q):
        whole = fields.at[k, :, pl.ds(0, CHUNK), :]
        with jax.named_scope(f"wait_two#k={k}"):
            pltpu.make_async_copy(whole, whole, r2.at[k, q]).wait()

    edge_rows = pl.ds(pl.multiple_of(core * (HALO + SEG), HALO), HALO)

    def halo(k):
        to = (seg + 1 + 14 * core) % 16
        mine = pl.ds(pl.multiple_of(SEG - core * (SEG - HALO), HALO), HALO)
        return pltpu.make_async_remote_copy(
            src_ref=fields.at[k, :, mine, :],
            dst_ref=fields.at[k, :, edge_rows, :],
            send_sem=sh.at[k],
            recv_sem=rh.at[k],
            device_id=device(y, to % 2, core, to // 2),
            device_id_type=MESH,
        )

    def pass_on(k):
        arrival(k, first_chunk(core))
        halo(k).start()

    def boundary(k):
        near = pl.ds(pl.multiple_of(HALO + core * 7 * B, B), B)
        far = pl.ds(pl.multiple_of(HALO + B + core * 5 * B, B), B)
        for e in range(2):
            low = jnp.dot(edges[0], fields[k, e, near, :], preferred_element_type=jnp.float32)
            low += jnp.dot(edges[1], fields[k, e, far, :], preferred_element_type=jnp.float32)
            deep = jnp.dot(edges[2], fields[k, e, near, :], preferred_element_type=jnp.float32)
            low, deep = low.astype(jnp.bfloat16), deep.astype(jnp.bfloat16)
            at_low = pl.ds(pl.multiple_of((1 - core) * B, B), B)
            at_deep = pl.ds(pl.multiple_of(core * B, B), B)
            for m in range(2):
                columns = pl.ds(m * 2 * M + e * M, M)
                images[at_low, columns] = low[m * B : (m + 1) * B]
                images[at_deep, columns] = deep[m * B : (m + 1) * B]
        project(fields.at[k, :, edge_rows, :], True)

    def slot(k):
        arrival(k, second_chunk(core))
        if k + 1 < SLOTS_DEV:
            pass_on(k + 1)
        with jax.named_scope(f"wait_halo#k={k}"):
            halo(k).wait_recv()
        with jax.named_scope(f"boundary#k={k}"):
            boundary(k)
        arrival(k, 1)
        with jax.named_scope(f"process#k={k}#q=0"):
            process(k, 0)
        arrival(k, 2)
        with jax.named_scope(f"process#k={k}#q=1"):
            process(k, 1)
        with jax.named_scope(f"process#k={k}#q=2"):
            process(k, 2)
        with jax.named_scope(f"process#k={k}#q=3"):
            process(k, 3)
        with jax.named_scope(f"narrow#k={k}"):
            parts[k] = total[...].astype(jnp.bfloat16).reshape(4, 2, 64, 2 * WIDE)
        for dz in (2, 1, 3):
            stiff_first(k, dz).start()
        mass_first(k, 1).start()

        @pl.when(xl == owner(k))
        def _():
            pltpu.make_async_copy(
                parts.at[k, :, xh, :, pl.ds(WIDE, WIDE)], mass_in.at[k % 2, place], rm1.at[k % 2]
            ).start()

        @pl.when(xl != owner(k))
        def _():
            mass_first(k, 0).start()

    place = xh * 2 + xl

    def owner(k):
        return (k // 2 + core) % 2

    def stiff_first(k, dz):
        z_ = (z + dz) % 4
        return pltpu.make_async_remote_copy(
            src_ref=parts.at[k, z_, :, :, pl.ds(0, WIDE)],
            dst_ref=stiff_in.at[k, 3 - dz],
            send_sem=sk1.at[k],
            recv_sem=rk1.at[k],
            device_id=device(y, xl, core, z_ * 2 + xh),
            device_id_type=MESH,
        )

    def stiff_second(k, dh):
        xh_ = (xh + dh) % 2
        return pltpu.make_async_remote_copy(
            src_ref=stiff_mid.at[k, xh_],
            dst_ref=stiff_end.at[k % 2, place],
            send_sem=sk2.at[k, dh],
            recv_sem=rk2.at[k % 2],
            device_id=device(y, owner(k), core, z * 2 + xh_),
            device_id_type=MESH,
        )

    def mass_first(k, dh):
        xh_ = (xh + dh) % 2
        return pltpu.make_async_remote_copy(
            src_ref=parts.at[k, :, xh_, :, pl.ds(WIDE, WIDE)],
            dst_ref=mass_in.at[k % 2, place],
            send_sem=sm1.at[k, dh],
            recv_sem=rm1.at[k % 2],
            device_id=device(y, owner(k), core, z * 2 + xh_),
            device_id_type=MESH,
        )

    def mass_second(k, dz):
        z_ = (z + dz) % 4
        return pltpu.make_async_remote_copy(
            src_ref=mass_mid.at[k % 2, z_],
            dst_ref=mass_end.at[k % 2, 3 - dz],
            send_sem=sm2.at[k % 2],
            recv_sem=rm2.at[k % 2],
            device_id=device(y, xl, core, z_ * 2 + xh),
            device_id_type=MESH,
        )

    def whole(ref, sem):
        pltpu.make_async_copy(ref, ref, sem).wait()

    def second(k):
        with jax.named_scope(f"wait_stiff#k={k}"):
            whole(stiff_in.at[k], rk1.at[k])
        acc = parts[k, z, :, :, pl.ds(0, WIDE)].astype(jnp.float32)
        for n in range(3):
            acc += stiff_in[k, n].astype(jnp.float32)
        stiff_mid[k] = acc.astype(jnp.bfloat16)
        stiff_second(k, 1).start()

        @pl.when(xl == owner(k))
        def _():
            pltpu.make_async_copy(
                stiff_mid.at[k, xh], stiff_end.at[k % 2, place], rk2.at[k % 2]
            ).start()
            with jax.named_scope(f"wait_mass#k={k}"):
                whole(mass_in.at[k % 2], rm1.at[k % 2])
            acc = mass_in[k % 2, 0].astype(jnp.float32)
            for n in range(1, 4):
                acc += mass_in[k % 2, n].astype(jnp.float32)
            mass_mid[k % 2] = acc.astype(jnp.bfloat16)
            for dz in (2, 1, 3):
                mass_second(k, dz).start()

        @pl.when(xl != owner(k))
        def _():
            stiff_second(k, 0).start()

    for k in range(SLOTS_DEV):
        if k + 2 < SLOTS_DEV:
            send_slot(k + 2)
        if k == 0:
            pass_on(0)
        slot(k)
        if k in (1, 2):
            second(k - 1)
    for k in range(SLOTS_DEV):
        if k + 1 not in (1, 2):
            second(k)

    for k in range(2):
        with jax.named_scope(f"wait_end#k={k}"):
            whole(stiff_end.at[k], rk2.at[k])
            whole(mass_end.at[k], rm2.at[k])
        acc = stiff_end[k, 0].astype(jnp.float32)
        for n in range(1, 4):
            acc += stiff_end[k, n].astype(jnp.float32)
        result[0, k] = acc
        acc = mass_mid[k, z].astype(jnp.float32)
        for n in range(3):
            acc += mass_end[k, n].astype(jnp.float32)
        result[1, k] = acc

    final = pltpu.make_async_copy(result, out, done)
    final.start()
    for q in range(NCHUNK):
        gone = arrived.at[q, pl.ds(0, 60)]
        pltpu.make_async_copy(gone, gone, s1.at[q]).wait()
    for k in range(SLOTS_DEV):
        gone = sent.at[pl.ds(0, 4), pl.ds(0, 14)]
        pltpu.make_async_copy(gone, gone, s2.at[k]).wait()
        halo(k).wait_send()
        whole(stiff_in.at[k], sk1.at[k])
        stiff_second(k, 1).wait_send()
        mass_first(k, 1).wait_send()

        @pl.when(xl != owner(k))
        def _():
            stiff_second(k, 0).wait_send()
            mass_first(k, 0).wait_send()

    for k in range(2):
        whole(mass_end.at[k], sm2.at[k])
    final.wait()


def per_device(psi_sectors, stiff_blocks, mass_blocks, harmonic_table):
    anywhere = pl.BlockSpec(memory_space=pl.ANY)
    vmem = pl.BlockSpec(memory_space=pltpu.VMEM)
    bf16, f32 = jnp.bfloat16, jnp.float32
    dma = pltpu.SemaphoreType.DMA
    out = pl.pallas_call(
        kernel,
        out_shape=jax.ShapeDtypeStruct((2, 2, 64, 512), f32),
        in_specs=[anywhere, anywhere, anywhere, pl.BlockSpec(memory_space=pltpu.SMEM)],
        out_specs=pl.BlockSpec(memory_space=pl.ANY),
        scratch_shapes=[
            pltpu.VMEM((NCHUNK, 64, PIECE, M), bf16),
            pltpu.VMEM((NCHUNK, 64, PIECE, M), bf16),
            pltpu.VMEM((SLOTS_DEV, 2, SEG + 2 * HALO, M), bf16),
            pltpu.VMEM((2, 1024, 1024), bf16),
            pltpu.VMEM((8, 2 * B, NBAND * B), bf16),
            pltpu.VMEM((3, 2 * B, B), bf16),
            pltpu.VMEM((CHUNK, 4 * M), bf16),
            pltpu.VMEM((2 * M, 4 * M), f32),
            pltpu.VMEM((SLOTS_DEV, 4, 2, 64, 2 * WIDE), bf16),
            pltpu.VMEM((SLOTS_DEV, 3, 2, 64, WIDE), bf16),
            pltpu.VMEM((SLOTS_DEV, 2, 64, WIDE), bf16),
            pltpu.VMEM((2, 4, 64, WIDE), bf16),
            pltpu.VMEM((2, 4, 4, 64, WIDE), bf16),
            pltpu.VMEM((2, 4, 64, WIDE), bf16),
            pltpu.VMEM((2, 3, 64, WIDE), bf16),
            pltpu.VMEM((2, 2, 64, WIDE), f32),
            dma,
            dma((2, NBAND)),
            dma((NCHUNK,)),
            dma((NCHUNK,)),
            dma((SLOTS_DEV,)),
            dma((SLOTS_DEV, NCHUNK)),
            dma((SLOTS_DEV,)),
            dma((SLOTS_DEV,)),
            dma((SLOTS_DEV,)),
            dma((SLOTS_DEV,)),
            dma((SLOTS_DEV, 2)),
            dma((2,)),
            dma((SLOTS_DEV, 2)),
            dma((2,)),
            dma((2,)),
            dma((2,)),
        ],
        compiler_params=pltpu.CompilerParams(
            collective_id=0, has_side_effects=True, vmem_limit_bytes=52 * 1024 * 1024
        ),
        name="reduce_sectors",
    )(psi_sectors, stiff_blocks, mass_blocks, harmonic_table)
    return out[0], out[1]


def solution(mesh):
    placed = (P("sector", "row", None), P("row", None, None, None), P("row", None, None, None), P())
    return jax.shard_map(
        per_device,
        mesh=mesh,
        in_specs=placed,
        out_specs=(P("sector", "row", None), P("sector", "row", None)),
        check_vma=False,
    )
```

```python
import functools
import math

import jax
import jax.numpy as jnp
from jax import lax
from jax.experimental import pallas as pl
from jax.experimental.pallas import tpu as pltpu
from jax.sharding import PartitionSpec as P

MESH = pl.DeviceIdType.MESH
B = 128
M = 256
NBAND = 5
ROWS_DEV = 2048
SEG = 1024
CHUNK = 256
NCHUNK = 4
PIECE = 32
TILE = 16
SLOTS_DEV = 4
LAST = SLOTS_DEV - 1
ORDER = (3, 0, 1, 2)
HALO = 256
WIDE = 512
SECTORS = 64
SLOTS = 32
SECTOR_OFFSETS = tuple(
    (dy, dx, dc) for dy in (2, 1, 3, 0) for dx in (1, 0) for dc in (0, 1) if dy or dx or dc
)
OWNER_OFFSETS = tuple((dy, dc) for dy in (2, 1, 3, 0) for dc in (0, 1) if dy or dc)


def coefficients(table):
    shape = (2 * SLOTS, SECTORS)
    line = lax.broadcasted_iota(jnp.int32, shape, 0)
    sector = lax.broadcasted_iota(jnp.int32, shape, 1)
    pair = jnp.zeros(shape, jnp.int32)
    for j in range(SLOTS):
        pair = jnp.where(line % SLOTS == j, table[j], pair)
    first = line < SLOTS
    zero = pair == 0
    freq = jnp.where(jnp.logical_and(zero, jnp.logical_not(first)), SECTORS // 2, pair)
    shift = jnp.where(jnp.logical_or(first, zero), 0, 3 * SECTORS // 4)
    phase = (freq * sector + shift) % SECTORS
    wave = jnp.cos(phase.astype(jnp.float32) * (2.0 * math.pi / SECTORS))
    return jnp.where(zero, math.sqrt(1.0 / SECTORS), math.sqrt(2.0 / SECTORS)) * wave


def kernel(
    psi, stiff, mass, table, out,
    arrived, sent, fields, lift, bands, edges, images, total, parts,
    stiff_in, stiff_mid, stiff_end, mass_in, mass_mid, mass_end, result, done,
    load_sem, s1, r1, s2, r2, rc, sh, rh, sk1, rk1, sk2, rk2, sm1, rm1, sm2, rm2,
):
    sec = lax.axis_index("sector")
    row = lax.axis_index("row")
    y, xl, core = sec // 4, (sec // 2) % 2, sec % 2
    turn = y * 2 + core
    seg = row * 2 + xl
    z, xh = row // 2, row % 2

    def device(y_, xl_, core_, row_):
        return {"sector": y_ * 4 + xl_ * 2 + core_, "row": row_}

    loads = []
    for m, src in enumerate((stiff, mass)):
        for k in range(NBAND):
            copy = pltpu.make_async_copy(
                src.at[pl.ds(pl.multiple_of(xl * 8, 8), 8), k],
                bands.at[:, pl.ds(m * B, B), pl.ds(k * B, B)],
                load_sem.at[m, k],
            )
            copy.start()
            loads.append(copy)

    barrier = pltpu.get_barrier_semaphore()
    count = 0
    for dy, dx, dc in SECTOR_OFFSETS:
        pl.semaphore_signal(
            barrier, inc=1, device_id_type=MESH,
            device_id=device((y + dy) % 4, (xl + dx) % 2, (core + dc) % 2, row),
        )
        count += 1
    for dr in range(1, 8):
        for dx in range(2):
            pl.semaphore_signal(
                barrier, inc=1, device_id_type=MESH,
                device_id=device(y, (xl + dx) % 2, core, (row + dr) % 8),
            )
            count += 1
    with jax.named_scope("barrier"):
        pl.semaphore_wait(barrier, count)

    def rows_of(xl_, turn_, q):
        return pl.ds(pl.multiple_of(xl_ * SEG + q * CHUNK + turn_ * PIECE, PIECE), PIECE)

    for q in ORDER:
        for dy, dx, dc in SECTOR_OFFSETS:
            y_, xl_, core_ = (y + dy) % 4, (xl + dx) % 2, (core + dc) % 2
            pltpu.make_async_remote_copy(
                src_ref=psi.at[:, rows_of(xl_, y_ * 2 + core_, q), :],
                dst_ref=arrived.at[q, pl.ds(sec * 4, 4)],
                send_sem=s1.at[q],
                recv_sem=r1.at[q],
                device_id=device(y_, xl_, core_, row),
                device_id_type=MESH,
            ).start()
        pltpu.make_async_copy(
            psi.at[:, rows_of(xl, turn, q), :], arrived.at[q, pl.ds(sec * 4, 4)], r1.at[q]
        ).start()

    coef = coefficients(table)
    coef_hi = coef.astype(jnp.bfloat16)
    coef_lo = (coef - coef_hi.astype(jnp.float32)).astype(jnp.bfloat16)
    quarter = 256

    def spread(n, _):
        i = lax.broadcasted_iota(jnp.int32, (quarter, 64), 0) + n * quarter
        g = i // TILE
        e, t, k = g % 2, (g // 2) % 8, g // 16
        slot = (t // 2) * 8 + ((k // 2 + t) % 2) * 4 + (t % 2) * 2 + k % 2
        want = e * 32 + slot
        pick = (lax.broadcasted_iota(jnp.int32, (quarter, 64), 1) == want).astype(jnp.bfloat16)
        col = lax.broadcasted_iota(jnp.int32, (64, 1024), 1) // TILE
        wide = (lax.broadcasted_iota(jnp.int32, (64, 1024), 0) == col).astype(jnp.bfloat16)
        same = (
            lax.broadcasted_iota(jnp.int32, (quarter, 1024), 0) % TILE
            == lax.broadcasted_iota(jnp.int32, (quarter, 1024), 1) % TILE
        )
        for h, part in enumerate((coef_hi, coef_lo)):
            chosen = jnp.dot(pick, part, preferred_element_type=jnp.float32).astype(jnp.bfloat16)
            full = jnp.dot(chosen, wide, preferred_element_type=jnp.float32)
            lift[h, pl.ds(pl.multiple_of(n * quarter, quarter), quarter), :] = jnp.where(
                same, full, 0.0
            ).astype(jnp.bfloat16)
        return 0

    with jax.named_scope("spread"):
        lax.fori_loop(0, 4, spread, 0)

    def mine(q):
        return pl.ds(pl.multiple_of(HALO + q * CHUNK + turn * PIECE, PIECE), PIECE)

    def send_fields(k, chunk):
        for dy, dc in OWNER_OFFSETS:
            y_, core_ = (y + dy) % 4, (core + dc) % 2
            q = chunk(core_)
            pltpu.make_async_remote_copy(
                src_ref=sent.at[q, pl.ds(k * 16 + (y_ * 2 + core_) * 2, 2)],
                dst_ref=fields.at[k, :, mine(q), :],
                send_sem=s2.at[k],
                recv_sem=r2.at[k, q],
                device_id=device(y_, xl, core_, row),
                device_id_type=MESH,
            ).start()
        q = chunk(core)
        pltpu.make_async_copy(
            sent.at[q, pl.ds(k * 16 + turn * 2, 2)], fields.at[k, :, mine(q), :], r2.at[k, q]
        ).start()

    def first_chunk(core_):
        return 3 * (1 - core_)

    def second_chunk(core_):
        return 3 * core_

    def send_slot(k):
        send_fields(k, second_chunk)
        if k + 1 < SLOTS_DEV:
            send_fields(k + 1, first_chunk)
        for step in range(2):
            for q in (1, 2):
                send_component(k, q, step)

    def send_component(k, q, step):
        for dy, dc in OWNER_OFFSETS:
            y_, core_ = (y + dy) % 4, (core + dc) % 2
            e = (step + core_) % 2
            pltpu.make_async_remote_copy(
                src_ref=sent.at[q, k * 16 + (y_ * 2 + core_) * 2 + e],
                dst_ref=fields.at[k, e, mine(q), :],
                send_sem=s2.at[k],
                recv_sem=rc.at[k, q - 1, step],
                device_id=device(y_, xl, core_, row),
                device_id_type=MESH,
            ).start()
        e = (step + core) % 2
        pltpu.make_async_copy(
            sent.at[q, k * 16 + turn * 2 + e], fields.at[k, e, mine(q), :], rc.at[k, q - 1, step]
        ).start()

    for q in ORDER:
        with jax.named_scope(f"wait_one#q={q}"):
            pltpu.make_async_copy(arrived.at[q], arrived.at[q], r1.at[q]).wait()

        def transform(h, _):
            rows = pl.ds(pl.multiple_of(h * TILE, TILE), TILE)
            x = arrived[q, :, rows, :].reshape(64 * TILE, M)
            for n in range(2):
                at = pl.ds(n * 512, 512)
                out = jnp.dot(lift[0, at, :], x, preferred_element_type=jnp.float32)
                out += jnp.dot(lift[1, at, :], x, preferred_element_type=jnp.float32)
                sent[q, pl.ds(n * 32, 32), rows, :] = out.astype(jnp.bfloat16).reshape(
                    32, TILE, M
                )
            return 0

        with jax.named_scope(f"transform#q={q}"):
            lax.fori_loop(0, PIECE // TILE, transform, 0)
        if q in (1, 2):
            for step in range(2):
                send_component(0, q, step)
        else:
            send_fields(0, lambda core_: q)
        if q == 0:
            send_fields(1, first_chunk)
    send_slot(1)

    for copy in loads:
        copy.wait()

    blank = pl.ds(pl.multiple_of((1 - core) * (HALO + SEG), HALO), HALO)
    for k in range(SLOTS_DEV):
        fields[k, :, blank, :] = jnp.zeros((2, HALO, M), jnp.bfloat16)
    near_block, far_block = core * 7, 1 + core * 5
    for n, (block, lane) in enumerate(
        ((near_block, B + core * 2 * B), (far_block, core * 4 * B), (near_block, core * 4 * B))
    ):
        for m in range(2):
            piece = bands[block, pl.ds(m * B, B), pl.ds(pl.multiple_of(lane, B), B)]
            edges[n, pl.ds(m * B, B), :] = piece.astype(jnp.float32).T.astype(jnp.bfloat16)

    def across_rows(left, right):
        return lax.dot_general(
            left, right, (((0,), (0,)), ((), ())), preferred_element_type=jnp.float32
        )

    def project(rows, first):
        for e in range(2):
            part = across_rows(rows[e], images[pl.ds(0, CHUNK), :])
            at = pl.ds(e * M, M)
            if first:
                total[at, :] = part
            else:
                total[at, :] += part

    def arrival(k, q):
        whole = fields.at[k, :, pl.ds(0, CHUNK), :]
        with jax.named_scope(f"wait_two#k={k}"):
            pltpu.make_async_copy(whole, whole, r2.at[k, q]).wait()

    edge_rows = pl.ds(pl.multiple_of(core * (HALO + SEG), HALO), HALO)

    def halo(k):
        to = (seg + 1 + 14 * core) % 16
        mine = pl.ds(pl.multiple_of(SEG - core * (SEG - HALO), HALO), HALO)
        return pltpu.make_async_remote_copy(
            src_ref=fields.at[k, :, mine, :],
            dst_ref=fields.at[k, :, edge_rows, :],
            send_sem=sh.at[k],
            recv_sem=rh.at[k],
            device_id=device(y, to % 2, core, to // 2),
            device_id_type=MESH,
        )

    def pass_on(k):
        arrival(k, first_chunk(core))
        halo(k).start()

    def boundary(k):
        near = pl.ds(pl.multiple_of(HALO + core * 7 * B, B), B)
        far = pl.ds(pl.multiple_of(HALO + B + core * 5 * B, B), B)
        for e in range(2):
            low = jnp.dot(edges[0], fields[k, e, near, :], preferred_element_type=jnp.float32)
            low += jnp.dot(edges[1], fields[k, e, far, :], preferred_element_type=jnp.float32)
            deep = jnp.dot(edges[2], fields[k, e, near, :], preferred_element_type=jnp.float32)
            low, deep = low.astype(jnp.bfloat16), deep.astype(jnp.bfloat16)
            at_low = pl.ds(pl.multiple_of((1 - core) * B, B), B)
            at_deep = pl.ds(pl.multiple_of(core * B, B), B)
            for m in range(2):
                columns = pl.ds(m * 2 * M + e * M, M)
                images[at_low, columns] = low[m * B : (m + 1) * B]
                images[at_deep, columns] = deep[m * B : (m + 1) * B]
        project(fields.at[k, :, edge_rows, :], True)

    def slot(k):
        own, other = core, 1 - core

        def lanes(start, e):
            return pl.ds(pl.multiple_of(start + e * M, M), M)

        def widen(q, e):
            for b in range(2):
                i = 2 * q + b
                window = fields[k, e, pl.ds(i * B, NBAND * B), :]
                w = jnp.dot(bands[i], window, preferred_element_type=jnp.float32)
                w = w.astype(jnp.bfloat16)
                images[pl.ds(i * B, B), lanes(0, e)] = w[:B]
                images[pl.ds(i * B, B), lanes(2 * M, e)] = w[B:]

        def add(chunks, e, columns):
            start, size = chunks[0] * CHUNK, len(chunks) * CHUNK
            left = fields[k, e, pl.ds(HALO + start, size), :]
            for at in columns:
                total[lanes(0, e), at] += across_rows(left, images[pl.ds(start, size), at])

        def component(q, step):
            whole(fields.at[k, 0, pl.ds(0, CHUNK), :], rc.at[k, q - 1, step])

        def first_half(*chunks):
            for q in chunks:
                widen(q, own)
            add(chunks, own, (lanes(0, own), lanes(2 * M, own)))

        def second_half(*chunks):
            for q in chunks:
                widen(q, other)
            add(chunks, own, (lanes(0, other), lanes(2 * M, other)))
            add(chunks, other, (pl.ds(0, 4 * M),))

        def narrow(e, at, width):
            parts[k, pl.ds(2 * e, 2), :, :, at] = (
                total[lanes(0, e), at].astype(jnp.bfloat16).reshape(2, 2, 64, width)
            )

        arrival(k, second_chunk(core))
        if k < LAST:
            pass_on(k + 1)
        halo(k).wait_recv()
        boundary(k)
        with jax.named_scope(f"component#k={k}#q=1#n=0"):
            component(1, 0)
        first_half(0)
        with jax.named_scope(f"component#k={k}#q=2#n=0"):
            component(2, 0)
        with jax.named_scope(f"first_half#k={k}"):
            first_half(1, 2, 3)
            for m in range(2):
                narrow(own, lanes(m * 2 * M, own), M)
        send_sums(k, ((own, own),))
        with jax.named_scope(f"component#k={k}#q=1#n=1"):
            component(1, 1)
        second_half(0)
        with jax.named_scope(f"component#k={k}#q=2#n=1"):
            component(2, 1)
        with jax.named_scope(f"second_half#k={k}"):
            second_half(1, 2, 3)
            for m in range(2):
                narrow(own, lanes(m * 2 * M, other), M)
            narrow(other, pl.ds(0, 4 * M), 4 * M)
        send_sums(k, ((own, other), (other, None)))

    def send_sums(k, blocks):
        def lanes(start, e):
            if e is None:
                return pl.ds(start, WIDE)
            return pl.ds(pl.multiple_of(start + e * M, M), M)

        for rows_e, cols_e in blocks:
            for dz in (2, 1, 3):
                z_ = (z + dz) % 4

                @pl.when(z_ // 2 == rows_e)
                def _():
                    pltpu.make_async_remote_copy(
                        src_ref=parts.at[k, z_, :, :, lanes(0, cols_e)],
                        dst_ref=stiff_in.at[k, 3 - dz, :, :, lanes(0, cols_e)],
                        send_sem=sk1.at[k],
                        recv_sem=rk1.at[k],
                        device_id=device(y, xl, core, z_ * 2 + xh),
                        device_id_type=MESH,
                    ).start()

            planes = pl.ds(2 * rows_e, 2)

            def to_owner(dh):
                xh_ = (xh + dh) % 2
                return pltpu.make_async_remote_copy(
                    src_ref=parts.at[k, planes, xh_, :, lanes(WIDE, cols_e)],
                    dst_ref=mass_in.at[k % 2, place, planes, :, lanes(0, cols_e)],
                    send_sem=sm1.at[k, dh],
                    recv_sem=rm1.at[k % 2],
                    device_id=device(y, owner(k), core, z * 2 + xh_),
                    device_id_type=MESH,
                )

            to_owner(1).start()

            @pl.when(xl == owner(k))
            def _():
                pltpu.make_async_copy(
                    parts.at[k, planes, xh, :, lanes(WIDE, cols_e)],
                    mass_in.at[k % 2, place, planes, :, lanes(0, cols_e)],
                    rm1.at[k % 2],
                ).start()

            @pl.when(xl != owner(k))
            def _():
                to_owner(0).start()

    place = xh * 2 + xl

    def owner(k):
        return (k // 2 + core) % 2

    def stiff_second(k, dh):
        xh_ = (xh + dh) % 2
        return pltpu.make_async_remote_copy(
            src_ref=stiff_mid.at[k, xh_],
            dst_ref=stiff_end.at[k % 2, place],
            send_sem=sk2.at[k, dh],
            recv_sem=rk2.at[k % 2],
            device_id=device(y, owner(k), core, z * 2 + xh_),
            device_id_type=MESH,
        )

    def mass_first(k, dh):
        xh_ = (xh + dh) % 2
        return pltpu.make_async_remote_copy(
            src_ref=parts.at[k, :, xh_, :, pl.ds(WIDE, WIDE)],
            dst_ref=mass_in.at[k % 2, place],
            send_sem=sm1.at[k, dh],
            recv_sem=rm1.at[k % 2],
            device_id=device(y, owner(k), core, z * 2 + xh_),
            device_id_type=MESH,
        )

    def mass_second(k, dz):
        z_ = (z + dz) % 4
        return pltpu.make_async_remote_copy(
            src_ref=mass_mid.at[k % 2, z_],
            dst_ref=mass_end.at[k % 2, 3 - dz],
            send_sem=sm2.at[k % 2],
            recv_sem=rm2.at[k % 2],
            device_id=device(y, xl, core, z_ * 2 + xh),
            device_id_type=MESH,
        )

    def whole(ref, sem):
        pltpu.make_async_copy(ref, ref, sem).wait()

    def second(k):
        with jax.named_scope(f"wait_stiff#k={k}"):
            whole(stiff_in.at[k], rk1.at[k])
        acc = parts[k, z, :, :, pl.ds(0, WIDE)].astype(jnp.float32)
        for n in range(3):
            acc += stiff_in[k, n].astype(jnp.float32)
        stiff_mid[k] = acc.astype(jnp.bfloat16)
        stiff_second(k, 1).start()

        @pl.when(xl == owner(k))
        def _():
            pltpu.make_async_copy(
                stiff_mid.at[k, xh], stiff_end.at[k % 2, place], rk2.at[k % 2]
            ).start()
            with jax.named_scope(f"wait_mass#k={k}"):
                whole(mass_in.at[k % 2], rm1.at[k % 2])
            acc = mass_in[k % 2, 0].astype(jnp.float32)
            for n in range(1, 4):
                acc += mass_in[k % 2, n].astype(jnp.float32)
            mass_mid[k % 2] = acc.astype(jnp.bfloat16)
            for dz in (2, 1, 3):
                mass_second(k, dz).start()

        @pl.when(xl != owner(k))
        def _():
            stiff_second(k, 0).start()

    for k in range(SLOTS_DEV):
        if k + 2 < SLOTS_DEV:
            send_slot(k + 2)
        if k == 0:
            pass_on(0)
        slot(k)
        if k in (1, 2):
            second(k - 1)
    for k in range(SLOTS_DEV):
        if k + 1 not in (1, 2):
            second(k)

    for k in range(2):
        with jax.named_scope(f"wait_end#k={k}"):
            whole(stiff_end.at[k], rk2.at[k])
            whole(mass_end.at[k], rm2.at[k])
        acc = stiff_end[k, 0].astype(jnp.float32)
        for n in range(1, 4):
            acc += stiff_end[k, n].astype(jnp.float32)
        result[0, k] = acc
        acc = mass_mid[k, z].astype(jnp.float32)
        for n in range(3):
            acc += mass_end[k, n].astype(jnp.float32)
        result[1, k] = acc

    final = pltpu.make_async_copy(result, out, done)
    final.start()
    for q in range(NCHUNK):
        gone = arrived.at[q, pl.ds(0, 60)]
        pltpu.make_async_copy(gone, gone, s1.at[q]).wait()
    for k in range(SLOTS_DEV):
        gone = sent.at[pl.ds(0, 4), pl.ds(0, 14)]
        pltpu.make_async_copy(gone, gone, s2.at[k]).wait()
        halo(k).wait_send()
        whole(stiff_in.at[k], sk1.at[k])
        stiff_second(k, 1).wait_send()
        mass_first(k, 1).wait_send()

        @pl.when(xl != owner(k))
        def _():
            stiff_second(k, 0).wait_send()
            mass_first(k, 0).wait_send()

    for k in range(2):
        whole(mass_end.at[k], sm2.at[k])
    final.wait()


def per_device(psi_sectors, stiff_blocks, mass_blocks, harmonic_table):
    anywhere = pl.BlockSpec(memory_space=pl.ANY)
    vmem = pl.BlockSpec(memory_space=pltpu.VMEM)
    bf16, f32 = jnp.bfloat16, jnp.float32
    dma = pltpu.SemaphoreType.DMA
    out = pl.pallas_call(
        kernel,
        out_shape=jax.ShapeDtypeStruct((2, 2, 64, 512), f32),
        in_specs=[anywhere, anywhere, anywhere, pl.BlockSpec(memory_space=pltpu.SMEM)],
        out_specs=pl.BlockSpec(memory_space=pl.ANY),
        scratch_shapes=[
            pltpu.VMEM((NCHUNK, 64, PIECE, M), bf16),
            pltpu.VMEM((NCHUNK, 64, PIECE, M), bf16),
            pltpu.VMEM((SLOTS_DEV, 2, SEG + 2 * HALO, M), bf16),
            pltpu.VMEM((2, 1024, 1024), bf16),
            pltpu.VMEM((8, 2 * B, NBAND * B), bf16),
            pltpu.VMEM((3, 2 * B, B), bf16),
            pltpu.VMEM((SEG, 4 * M), bf16),
            pltpu.VMEM((2 * M, 4 * M), f32),
            pltpu.VMEM((SLOTS_DEV, 4, 2, 64, 2 * WIDE), bf16),
            pltpu.VMEM((SLOTS_DEV, 3, 2, 64, WIDE), bf16),
            pltpu.VMEM((SLOTS_DEV, 2, 64, WIDE), bf16),
            pltpu.VMEM((2, 4, 64, WIDE), bf16),
            pltpu.VMEM((2, 4, 4, 64, WIDE), bf16),
            pltpu.VMEM((2, 4, 64, WIDE), bf16),
            pltpu.VMEM((2, 3, 64, WIDE), bf16),
            pltpu.VMEM((2, 2, 64, WIDE), f32),
            dma,
            dma((2, NBAND)),
            dma((NCHUNK,)),
            dma((NCHUNK,)),
            dma((SLOTS_DEV,)),
            dma((SLOTS_DEV, NCHUNK)),
            dma((SLOTS_DEV, 2, 2)),
            dma((SLOTS_DEV,)),
            dma((SLOTS_DEV,)),
            dma((SLOTS_DEV,)),
            dma((SLOTS_DEV,)),
            dma((SLOTS_DEV, 2)),
            dma((2,)),
            dma((SLOTS_DEV, 2)),
            dma((2,)),
            dma((2,)),
            dma((2,)),
        ],
        compiler_params=pltpu.CompilerParams(
            collective_id=0, has_side_effects=True, vmem_limit_bytes=52 * 1024 * 1024
        ),
        name="reduce_sectors",
    )(psi_sectors, stiff_blocks, mass_blocks, harmonic_table)
    return out[0], out[1]


def solution(mesh):
    placed = (P("sector", "row", None), P("row", None, None, None), P("row", None, None, None), P())
    return jax.shard_map(
        per_device,
        mesh=mesh,
        in_specs=placed,
        out_specs=(P("sector", "row", None), P("sector", "row", None)),
        check_vma=False,
    )
```

```python
import functools
import math

import jax
import jax.numpy as jnp
from jax import lax
from jax.experimental import pallas as pl
from jax.experimental.pallas import tpu as pltpu
from jax.sharding import PartitionSpec as P

MESH = pl.DeviceIdType.MESH
B = 128
M = 256
NBAND = 5
ROWS_DEV = 2048
SEG = 1024
CHUNK = 256
NCHUNK = 4
PIECE = 32
TILE = 16
SLOTS_DEV = 4
LAST = SLOTS_DEV - 1
ORDER = (3, 0, 1, 2)
HALO = 256
WIDE = 512
SECTORS = 64
SLOTS = 32
SECTOR_OFFSETS = tuple(
    (dy, dx, dc) for dy in (2, 1, 3, 0) for dx in (1, 0) for dc in (0, 1) if dy or dx or dc
)
OWNER_OFFSETS = tuple((dy, dc) for dy in (2, 1, 3, 0) for dc in (0, 1) if dy or dc)


def coefficients(table):
    shape = (2 * SLOTS, SECTORS)
    line = lax.broadcasted_iota(jnp.int32, shape, 0)
    sector = lax.broadcasted_iota(jnp.int32, shape, 1)
    pair = jnp.zeros(shape, jnp.int32)
    for j in range(SLOTS):
        pair = jnp.where(line % SLOTS == j, table[j], pair)
    first = line < SLOTS
    zero = pair == 0
    freq = jnp.where(jnp.logical_and(zero, jnp.logical_not(first)), SECTORS // 2, pair)
    shift = jnp.where(jnp.logical_or(first, zero), 0, 3 * SECTORS // 4)
    phase = (freq * sector + shift) % SECTORS
    wave = jnp.cos(phase.astype(jnp.float32) * (2.0 * math.pi / SECTORS))
    return jnp.where(zero, math.sqrt(1.0 / SECTORS), math.sqrt(2.0 / SECTORS)) * wave


def kernel(
    psi, stiff, mass, table_in, out,
    arrived, sent, fields, lift, bands, edges, images, total, parts,
    stiff_in, stiff_mid, stiff_end, mass_in, mass_mid, mass_end, table, table_sem,
    load_sem, s1, r1, s2, r2, rc, sh, rh, sk1, rk1, sk2, rk2, sm1, rm1, sm2, rm2,
):
    sec = lax.axis_index("sector")
    row = lax.axis_index("row")
    y, xl, core = sec // 4, (sec // 2) % 2, sec % 2
    turn = y * 2 + core
    seg = row * 2 + xl
    z, xh = row // 2, row % 2

    def device(y_, xl_, core_, row_):
        return {"sector": y_ * 4 + xl_ * 2 + core_, "row": row_}

    barrier = pltpu.get_barrier_semaphore()
    count = 0
    for dy, dx, dc in SECTOR_OFFSETS:
        pl.semaphore_signal(
            barrier, inc=1, device_id_type=MESH,
            device_id=device((y + dy) % 4, (xl + dx) % 2, (core + dc) % 2, row),
        )
        count += 1
    for dr in range(1, 8):
        for dx in range(2):
            pl.semaphore_signal(
                barrier, inc=1, device_id_type=MESH,
                device_id=device(y, (xl + dx) % 2, core, (row + dr) % 8),
            )
            count += 1
    table_copy = pltpu.make_async_copy(table_in, table, table_sem)
    table_copy.start()
    loads = []
    for m, src in enumerate((stiff, mass)):
        for k in range(NBAND):
            copy = pltpu.make_async_copy(
                src.at[pl.ds(pl.multiple_of(xl * 8, 8), 8), k],
                bands.at[:, pl.ds(m * B, B), pl.ds(k * B, B)],
                load_sem.at[m, k],
            )
            copy.start()
            loads.append(copy)

    with jax.named_scope("barrier"):
        pl.semaphore_wait(barrier, count)

    def rows_of(xl_, turn_, q):
        return pl.ds(pl.multiple_of(xl_ * SEG + q * CHUNK + turn_ * PIECE, PIECE), PIECE)

    for q in ORDER:
        for dy, dx, dc in SECTOR_OFFSETS:
            y_, xl_, core_ = (y + dy) % 4, (xl + dx) % 2, (core + dc) % 2
            pltpu.make_async_remote_copy(
                src_ref=psi.at[:, rows_of(xl_, y_ * 2 + core_, q), :],
                dst_ref=arrived.at[q, pl.ds(sec * 4, 4)],
                send_sem=s1.at[q],
                recv_sem=r1.at[q],
                device_id=device(y_, xl_, core_, row),
                device_id_type=MESH,
            ).start()
        pltpu.make_async_copy(
            psi.at[:, rows_of(xl, turn, q), :], arrived.at[q, pl.ds(sec * 4, 4)], r1.at[q]
        ).start()

    table_copy.wait()
    coef = coefficients(table)
    coef_hi = coef.astype(jnp.bfloat16)
    coef_lo = (coef - coef_hi.astype(jnp.float32)).astype(jnp.bfloat16)
    quarter = 256

    def spread(n, _):
        i = lax.broadcasted_iota(jnp.int32, (quarter, 64), 0) + n * quarter
        g = i // TILE
        e, t, k = g % 2, (g // 2) % 8, g // 16
        slot = (t // 2) * 8 + ((k // 2 + t) % 2) * 4 + (t % 2) * 2 + k % 2
        want = e * 32 + slot
        pick = (lax.broadcasted_iota(jnp.int32, (quarter, 64), 1) == want).astype(jnp.bfloat16)
        col = lax.broadcasted_iota(jnp.int32, (64, 1024), 1) // TILE
        wide = (lax.broadcasted_iota(jnp.int32, (64, 1024), 0) == col).astype(jnp.bfloat16)
        same = (
            lax.broadcasted_iota(jnp.int32, (quarter, 1024), 0) % TILE
            == lax.broadcasted_iota(jnp.int32, (quarter, 1024), 1) % TILE
        )
        for h, part in enumerate((coef_hi, coef_lo)):
            chosen = jnp.dot(pick, part, preferred_element_type=jnp.float32).astype(jnp.bfloat16)
            full = jnp.dot(chosen, wide, preferred_element_type=jnp.float32)
            lift[h, pl.ds(pl.multiple_of(n * quarter, quarter), quarter), :] = jnp.where(
                same, full, 0.0
            ).astype(jnp.bfloat16)
        return 0

    with jax.named_scope("spread"):
        lax.fori_loop(0, 4, spread, 0)

    def mine(q):
        return pl.ds(pl.multiple_of(HALO + q * CHUNK + turn * PIECE, PIECE), PIECE)

    def send_fields(k, chunk):
        for dy, dc in OWNER_OFFSETS:
            y_, core_ = (y + dy) % 4, (core + dc) % 2
            q = chunk(core_)
            pltpu.make_async_remote_copy(
                src_ref=sent.at[q, pl.ds(k * 16 + (y_ * 2 + core_) * 2, 2)],
                dst_ref=fields.at[k, :, mine(q), :],
                send_sem=s2.at[k],
                recv_sem=r2.at[k, q],
                device_id=device(y_, xl, core_, row),
                device_id_type=MESH,
            ).start()
        q = chunk(core)
        pltpu.make_async_copy(
            sent.at[q, pl.ds(k * 16 + turn * 2, 2)], fields.at[k, :, mine(q), :], r2.at[k, q]
        ).start()

    def first_chunk(core_):
        return 3 * (1 - core_)

    def second_chunk(core_):
        return 3 * core_

    def send_slot(k):
        send_fields(k, second_chunk)
        if k + 1 < SLOTS_DEV:
            send_fields(k + 1, first_chunk)
        for step in range(2):
            for q in (1, 2):
                send_component(k, q, step)

    def send_component(k, q, step):
        for dy, dc in OWNER_OFFSETS:
            y_, core_ = (y + dy) % 4, (core + dc) % 2
            e = (step + core_) % 2
            pltpu.make_async_remote_copy(
                src_ref=sent.at[q, k * 16 + (y_ * 2 + core_) * 2 + e],
                dst_ref=fields.at[k, e, mine(q), :],
                send_sem=s2.at[k],
                recv_sem=rc.at[k, q - 1, step],
                device_id=device(y_, xl, core_, row),
                device_id_type=MESH,
            ).start()
        e = (step + core) % 2
        pltpu.make_async_copy(
            sent.at[q, k * 16 + turn * 2 + e], fields.at[k, e, mine(q), :], rc.at[k, q - 1, step]
        ).start()

    for q in ORDER:
        with jax.named_scope(f"wait_one#q={q}"):
            pltpu.make_async_copy(arrived.at[q], arrived.at[q], r1.at[q]).wait()

        def transform(h, _):
            rows = pl.ds(pl.multiple_of(h * TILE, TILE), TILE)
            x = arrived[q, :, rows, :].reshape(64 * TILE, M)
            for n in range(2):
                at = pl.ds(n * 512, 512)
                out = jnp.dot(lift[0, at, :], x, preferred_element_type=jnp.float32)
                out += jnp.dot(lift[1, at, :], x, preferred_element_type=jnp.float32)
                sent[q, pl.ds(n * 32, 32), rows, :] = out.astype(jnp.bfloat16).reshape(
                    32, TILE, M
                )
            return 0

        with jax.named_scope(f"transform#q={q}"):
            lax.fori_loop(0, PIECE // TILE, transform, 0)
        if q in (1, 2):
            for step in range(2):
                send_component(0, q, step)
        else:
            send_fields(0, lambda core_: q)
        if q == 0:
            send_fields(1, first_chunk)
    send_slot(1)

    for copy in loads:
        copy.wait()

    blank = pl.ds(pl.multiple_of((1 - core) * (HALO + SEG), HALO), HALO)
    for k in range(SLOTS_DEV):
        fields[k, :, blank, :] = jnp.zeros((2, HALO, M), jnp.bfloat16)
    near_block, far_block = core * 7, 1 + core * 5
    for n, (block, lane) in enumerate(
        ((near_block, B + core * 2 * B), (far_block, core * 4 * B), (near_block, core * 4 * B))
    ):
        for m in range(2):
            piece = bands[block, pl.ds(m * B, B), pl.ds(pl.multiple_of(lane, B), B)]
            edges[n, pl.ds(m * B, B), :] = piece.astype(jnp.float32).T.astype(jnp.bfloat16)

    def across_rows(left, right):
        return lax.dot_general(
            left, right, (((0,), (0,)), ((), ())), preferred_element_type=jnp.float32
        )

    def project(rows, first):
        for e in range(2):
            part = across_rows(rows[e], images[pl.ds(0, CHUNK), :])
            at = pl.ds(e * M, M)
            if first:
                total[at, :] = part
            else:
                total[at, :] += part

    def arrival(k, q):
        whole = fields.at[k, :, pl.ds(0, CHUNK), :]
        with jax.named_scope(f"wait_two#k={k}"):
            pltpu.make_async_copy(whole, whole, r2.at[k, q]).wait()

    edge_rows = pl.ds(pl.multiple_of(core * (HALO + SEG), HALO), HALO)

    def halo(k):
        to = (seg + 1 + 14 * core) % 16
        mine = pl.ds(pl.multiple_of(SEG - core * (SEG - HALO), HALO), HALO)
        return pltpu.make_async_remote_copy(
            src_ref=fields.at[k, :, mine, :],
            dst_ref=fields.at[k, :, edge_rows, :],
            send_sem=sh.at[k],
            recv_sem=rh.at[k],
            device_id=device(y, to % 2, core, to // 2),
            device_id_type=MESH,
        )

    def pass_on(k):
        arrival(k, first_chunk(core))
        halo(k).start()

    def boundary(k):
        near = pl.ds(pl.multiple_of(HALO + core * 7 * B, B), B)
        far = pl.ds(pl.multiple_of(HALO + B + core * 5 * B, B), B)
        for e in range(2):
            low = jnp.dot(edges[0], fields[k, e, near, :], preferred_element_type=jnp.float32)
            low += jnp.dot(edges[1], fields[k, e, far, :], preferred_element_type=jnp.float32)
            deep = jnp.dot(edges[2], fields[k, e, near, :], preferred_element_type=jnp.float32)
            low, deep = low.astype(jnp.bfloat16), deep.astype(jnp.bfloat16)
            at_low = pl.ds(pl.multiple_of((1 - core) * B, B), B)
            at_deep = pl.ds(pl.multiple_of(core * B, B), B)
            for m in range(2):
                columns = pl.ds(m * 2 * M + e * M, M)
                images[at_low, columns] = low[m * B : (m + 1) * B]
                images[at_deep, columns] = deep[m * B : (m + 1) * B]
        project(fields.at[k, :, edge_rows, :], True)

    def slot(k):
        own, other = core, 1 - core

        def lanes(start, e):
            return pl.ds(pl.multiple_of(start + e * M, M), M)

        def widen(q, e):
            for b in range(2):
                i = 2 * q + b
                window = fields[k, e, pl.ds(i * B, NBAND * B), :]
                w = jnp.dot(bands[i], window, preferred_element_type=jnp.float32)
                w = w.astype(jnp.bfloat16)
                images[pl.ds(i * B, B), lanes(0, e)] = w[:B]
                images[pl.ds(i * B, B), lanes(2 * M, e)] = w[B:]

        def add(chunks, e, columns):
            start, size = chunks[0] * CHUNK, len(chunks) * CHUNK
            left = fields[k, e, pl.ds(HALO + start, size), :]
            for at in columns:
                total[lanes(0, e), at] += across_rows(left, images[pl.ds(start, size), at])

        def component(q, step):
            whole(fields.at[k, 0, pl.ds(0, CHUNK), :], rc.at[k, q - 1, step])

        def first_half(*chunks):
            for q in chunks:
                widen(q, own)
            add(chunks, own, (lanes(0, own), lanes(2 * M, own)))

        def second_half(*chunks):
            for q in chunks:
                widen(q, other)
            add(chunks, own, (lanes(0, other), lanes(2 * M, other)))

        def narrow(e, at, width):
            parts[k, pl.ds(2 * e, 2), :, :, at] = (
                total[lanes(0, e), at].astype(jnp.bfloat16).reshape(2, 2, 64, width)
            )

        arrival(k, second_chunk(core))
        if k < LAST:
            pass_on(k + 1)
        halo(k).wait_recv()
        boundary(k)
        with jax.named_scope(f"component#k={k}#q=1#n=0"):
            component(1, 0)
        first_half(0)
        with jax.named_scope(f"component#k={k}#q=2#n=0"):
            component(2, 0)
        with jax.named_scope(f"first_half#k={k}"):
            first_half(1, 2, 3)
            for m in range(2):
                narrow(own, lanes(m * 2 * M, own), M)
        send_sums(k, ((own, own),))
        with jax.named_scope(f"component#k={k}#q=1#n=1"):
            component(1, 1)
        second_half(0)
        add((0,), other, (pl.ds(0, 4 * M),))
        with jax.named_scope(f"component#k={k}#q=2#n=1"):
            component(2, 1)
        with jax.named_scope(f"second_half#k={k}"):
            second_half(1, 2, 3)
            for m in range(2):
                narrow(own, lanes(m * 2 * M, other), M)
        send_sums(k, ((own, other),))
        with jax.named_scope(f"third_part#k={k}"):
            add((1, 2, 3), other, (pl.ds(0, 4 * M),))
            narrow(other, pl.ds(0, 4 * M), 4 * M)
        send_sums(k, ((other, None),))

    def send_sums(k, blocks):
        def lanes(start, e):
            if e is None:
                return pl.ds(start, WIDE)
            return pl.ds(pl.multiple_of(start + e * M, M), M)

        for rows_e, cols_e in blocks:
            planes = pl.ds(2 * rows_e, 2)

            def to_owner(dh):
                xh_ = (xh + dh) % 2
                return pltpu.make_async_remote_copy(
                    src_ref=parts.at[k, planes, xh_, :, lanes(WIDE, cols_e)],
                    dst_ref=mass_in.at[k % 2, place, planes, :, lanes(0, cols_e)],
                    send_sem=sm1.at[k, dh],
                    recv_sem=rm1.at[k % 2],
                    device_id=device(y, owner(k), core, z * 2 + xh_),
                    device_id_type=MESH,
                )

            to_owner(1).start()

            @pl.when(xl == owner(k))
            def _():
                pltpu.make_async_copy(
                    parts.at[k, planes, xh, :, lanes(WIDE, cols_e)],
                    mass_in.at[k % 2, place, planes, :, lanes(0, cols_e)],
                    rm1.at[k % 2],
                ).start()

            @pl.when(xl != owner(k))
            def _():
                to_owner(0).start()

            for dz in (2, 1, 3):
                z_ = (z + dz) % 4

                @pl.when(z_ // 2 == rows_e)
                def _():
                    pltpu.make_async_remote_copy(
                        src_ref=parts.at[k, z_, :, :, lanes(0, cols_e)],
                        dst_ref=stiff_in.at[k, 3 - dz, :, :, lanes(0, cols_e)],
                        send_sem=sk1.at[k],
                        recv_sem=rk1.at[k],
                        device_id=device(y, xl, core, z_ * 2 + xh),
                        device_id_type=MESH,
                    ).start()

    place = xh * 2 + xl

    def owner(k):
        return (k // 2 + core) % 2

    def stiff_second(k, dh):
        xh_ = (xh + dh) % 2
        return pltpu.make_async_remote_copy(
            src_ref=stiff_mid.at[k, xh_],
            dst_ref=stiff_end.at[k % 2, place],
            send_sem=sk2.at[k, dh],
            recv_sem=rk2.at[k % 2],
            device_id=device(y, owner(k), core, z * 2 + xh_),
            device_id_type=MESH,
        )

    def mass_first(k, dh):
        xh_ = (xh + dh) % 2
        return pltpu.make_async_remote_copy(
            src_ref=parts.at[k, :, xh_, :, pl.ds(WIDE, WIDE)],
            dst_ref=mass_in.at[k % 2, place],
            send_sem=sm1.at[k, dh],
            recv_sem=rm1.at[k % 2],
            device_id=device(y, owner(k), core, z * 2 + xh_),
            device_id_type=MESH,
        )

    def mass_second(k, dz):
        z_ = (z + dz) % 4
        return pltpu.make_async_remote_copy(
            src_ref=mass_mid.at[k % 2, z_],
            dst_ref=mass_end.at[k % 2, 3 - dz],
            send_sem=sm2.at[k % 2],
            recv_sem=rm2.at[k % 2],
            device_id=device(y, xl, core, z_ * 2 + xh),
            device_id_type=MESH,
        )

    def whole(ref, sem):
        pltpu.make_async_copy(ref, ref, sem).wait()

    def second(k):
        with jax.named_scope(f"wait_stiff#k={k}"):
            whole(stiff_in.at[k], rk1.at[k])
        acc = parts[k, z, :, :, pl.ds(0, WIDE)].astype(jnp.float32)
        for n in range(3):
            acc += stiff_in[k, n].astype(jnp.float32)
        stiff_mid[k] = acc.astype(jnp.bfloat16)
        stiff_second(k, 1).start()

        @pl.when(xl == owner(k))
        def _():
            pltpu.make_async_copy(
                stiff_mid.at[k, xh], stiff_end.at[k % 2, place], rk2.at[k % 2]
            ).start()
            with jax.named_scope(f"wait_mass#k={k}"):
                whole(mass_in.at[k % 2], rm1.at[k % 2])
            acc = mass_in[k % 2, 0].astype(jnp.float32)
            for n in range(1, 4):
                acc += mass_in[k % 2, n].astype(jnp.float32)
            mass_mid[k % 2] = acc.astype(jnp.bfloat16)
            for dz in (2, 1, 3):
                mass_second(k, dz).start()

        @pl.when(xl != owner(k))
        def _():
            stiff_second(k, 0).start()

    for k in range(SLOTS_DEV):
        if k + 2 < SLOTS_DEV:
            send_slot(k + 2)
        if k == 0:
            pass_on(0)
        slot(k)
        if k in (1, 2):
            second(k - 1)
    for k in range(SLOTS_DEV):
        if k + 1 not in (1, 2):
            second(k)

    for q in range(NCHUNK):
        gone = arrived.at[q, pl.ds(0, 60)]
        pltpu.make_async_copy(gone, gone, s1.at[q]).wait()
    for k in range(SLOTS_DEV):
        gone = sent.at[pl.ds(0, 4), pl.ds(0, 14)]
        pltpu.make_async_copy(gone, gone, s2.at[k]).wait()
        halo(k).wait_send()
        whole(stiff_in.at[k], sk1.at[k])
        mass_first(k, 1).wait_send()

        @pl.when(xl != owner(k))
        def _():
            mass_first(k, 0).wait_send()

    for k in range(2):
        with jax.named_scope(f"wait_end#k={k}"):
            whole(stiff_end.at[k], rk2.at[k])
            whole(mass_end.at[k], rm2.at[k])
        acc = stiff_end[k, 0].astype(jnp.float32)
        for n in range(1, 4):
            acc += stiff_end[k, n].astype(jnp.float32)
        out[0, k] = acc
        acc = mass_mid[k, z].astype(jnp.float32)
        for n in range(3):
            acc += mass_end[k, n].astype(jnp.float32)
        out[1, k] = acc

    for k in range(SLOTS_DEV):
        stiff_second(k, 1).wait_send()

        @pl.when(xl != owner(k))
        def _():
            stiff_second(k, 0).wait_send()

    for k in range(2):
        whole(mass_end.at[k], sm2.at[k])


def per_device(psi_sectors, stiff_blocks, mass_blocks, harmonic_table):
    anywhere = pl.BlockSpec(memory_space=pl.ANY)
    vmem = pl.BlockSpec(memory_space=pltpu.VMEM)
    bf16, f32 = jnp.bfloat16, jnp.float32
    dma = pltpu.SemaphoreType.DMA
    out = pl.pallas_call(
        kernel,
        out_shape=jax.ShapeDtypeStruct((2, 2, 64, 512), f32),
        in_specs=[anywhere, anywhere, anywhere, anywhere],
        out_specs=pl.BlockSpec(memory_space=pltpu.VMEM),
        scratch_shapes=[
            pltpu.VMEM((NCHUNK, 64, PIECE, M), bf16),
            pltpu.VMEM((NCHUNK, 64, PIECE, M), bf16),
            pltpu.VMEM((SLOTS_DEV, 2, SEG + 2 * HALO, M), bf16),
            pltpu.VMEM((2, 1024, 1024), bf16),
            pltpu.VMEM((8, 2 * B, NBAND * B), bf16),
            pltpu.VMEM((3, 2 * B, B), bf16),
            pltpu.VMEM((SEG, 4 * M), bf16),
            pltpu.VMEM((2 * M, 4 * M), f32),
            pltpu.VMEM((SLOTS_DEV, 4, 2, 64, 2 * WIDE), bf16),
            pltpu.VMEM((SLOTS_DEV, 3, 2, 64, WIDE), bf16),
            pltpu.VMEM((SLOTS_DEV, 2, 64, WIDE), bf16),
            pltpu.VMEM((2, 4, 64, WIDE), bf16),
            pltpu.VMEM((2, 4, 4, 64, WIDE), bf16),
            pltpu.VMEM((2, 4, 64, WIDE), bf16),
            pltpu.VMEM((2, 3, 64, WIDE), bf16),
            pltpu.SMEM((SLOTS,), jnp.int32),
            dma,
            dma((2, NBAND)),
            dma((NCHUNK,)),
            dma((NCHUNK,)),
            dma((SLOTS_DEV,)),
            dma((SLOTS_DEV, NCHUNK)),
            dma((SLOTS_DEV, 2, 2)),
            dma((SLOTS_DEV,)),
            dma((SLOTS_DEV,)),
            dma((SLOTS_DEV,)),
            dma((SLOTS_DEV,)),
            dma((SLOTS_DEV, 2)),
            dma((2,)),
            dma((SLOTS_DEV, 2)),
            dma((2,)),
            dma((2,)),
            dma((2,)),
        ],
        compiler_params=pltpu.CompilerParams(
            collective_id=0, has_side_effects=True, vmem_limit_bytes=52 * 1024 * 1024
        ),
        name="reduce_sectors",
    )(psi_sectors, stiff_blocks, mass_blocks, harmonic_table)
    return out[0], out[1]


def solution(mesh):
    placed = (P("sector", "row", None), P("row", None, None, None), P("row", None, None, None), P())
    return jax.shard_map(
        per_device,
        mesh=mesh,
        in_specs=placed,
        out_specs=(P("sector", "row", None), P("sector", "row", None)),
        check_vma=False,
    )
```

```python
import functools
import math

import jax
import jax.numpy as jnp
from jax import lax
from jax.experimental import pallas as pl
from jax.experimental.pallas import tpu as pltpu
from jax.sharding import PartitionSpec as P

MESH = pl.DeviceIdType.MESH
B = 128
M = 256
NBAND = 5
ROWS_DEV = 2048
SEG = 1024
CHUNK = 256
NCHUNK = 4
PIECE = 32
TILE = 16
SLOTS_DEV = 4
LAST = SLOTS_DEV - 1
ORDER = (3, 0, 1, 2)
HALO = 256
WIDE = 512
SECTORS = 64
SLOTS = 32
SECTOR_OFFSETS = tuple(
    (dy, dx, dc) for dy in (2, 1, 3, 0) for dx in (1, 0) for dc in (0, 1) if dy or dx or dc
)
OWNER_OFFSETS = tuple((dy, dc) for dy in (2, 1, 3, 0) for dc in (0, 1) if dy or dc)


def coefficients(table):
    shape = (2 * SLOTS, SECTORS)
    line = lax.broadcasted_iota(jnp.int32, shape, 0)
    sector = lax.broadcasted_iota(jnp.int32, shape, 1)
    pair = jnp.zeros(shape, jnp.int32)
    for j in range(SLOTS):
        pair = jnp.where(line % SLOTS == j, table[j], pair)
    first = line < SLOTS
    zero = pair == 0
    freq = jnp.where(jnp.logical_and(zero, jnp.logical_not(first)), SECTORS // 2, pair)
    shift = jnp.where(jnp.logical_or(first, zero), 0, 3 * SECTORS // 4)
    phase = (freq * sector + shift) % SECTORS
    wave = jnp.cos(phase.astype(jnp.float32) * (2.0 * math.pi / SECTORS))
    return jnp.where(zero, math.sqrt(1.0 / SECTORS), math.sqrt(2.0 / SECTORS)) * wave


def kernel(
    psi, stiff, mass, table_in, out,
    arrived, sent, fields, lift, bands, edges, images, total, parts,
    stiff_in, stiff_mid, stiff_end, mass_in, mass_mid, mass_end, table, table_sem,
    load_sem, s1, r1, s2, r2, rc, sh, rh, sk1, rk1, sk2, rk2, sm1, rm1, sm2, rm2,
):
    sec = lax.axis_index("sector")
    row = lax.axis_index("row")
    y, xl, core = sec // 4, (sec // 2) % 2, sec % 2
    turn = y * 2 + core
    seg = row * 2 + xl
    z, xh = row // 2, row % 2

    def device(y_, xl_, core_, row_):
        return {"sector": y_ * 4 + xl_ * 2 + core_, "row": row_}

    barrier = pltpu.get_barrier_semaphore()
    count = 0
    for dy, dx, dc in SECTOR_OFFSETS:
        pl.semaphore_signal(
            barrier, inc=1, device_id_type=MESH,
            device_id=device((y + dy) % 4, (xl + dx) % 2, (core + dc) % 2, row),
        )
        count += 1
    for dr in range(1, 8):
        for dx in range(2):
            pl.semaphore_signal(
                barrier, inc=1, device_id_type=MESH,
                device_id=device(y, (xl + dx) % 2, core, (row + dr) % 8),
            )
            count += 1
    table_copy = pltpu.make_async_copy(table_in, table, table_sem)
    table_copy.start()
    loads = []
    for m, src in enumerate((stiff, mass)):
        for k in range(NBAND):
            copy = pltpu.make_async_copy(
                src.at[pl.ds(pl.multiple_of(xl * 8, 8), 8), k],
                bands.at[:, pl.ds(m * B, B), pl.ds(k * B, B)],
                load_sem.at[m, k],
            )
            copy.start()
            loads.append(copy)

    with jax.named_scope("barrier"):
        pl.semaphore_wait(barrier, count)

    def rows_of(xl_, turn_, q):
        return pl.ds(pl.multiple_of(xl_ * SEG + q * CHUNK + turn_ * PIECE, PIECE), PIECE)

    for q in ORDER:
        for dy, dx, dc in SECTOR_OFFSETS:
            y_, xl_, core_ = (y + dy) % 4, (xl + dx) % 2, (core + dc) % 2
            pltpu.make_async_remote_copy(
                src_ref=psi.at[:, rows_of(xl_, y_ * 2 + core_, q), :],
                dst_ref=arrived.at[q, pl.ds(sec * 4, 4)],
                send_sem=s1.at[q],
                recv_sem=r1.at[q],
                device_id=device(y_, xl_, core_, row),
                device_id_type=MESH,
            ).start()
        pltpu.make_async_copy(
            psi.at[:, rows_of(xl, turn, q), :], arrived.at[q, pl.ds(sec * 4, 4)], r1.at[q]
        ).start()

    table_copy.wait()
    coef = coefficients(table)
    coef_hi = coef.astype(jnp.bfloat16)
    coef_lo = (coef - coef_hi.astype(jnp.float32)).astype(jnp.bfloat16)
    quarter = 256

    def spread(n, _):
        i = lax.broadcasted_iota(jnp.int32, (quarter, 64), 0) + n * quarter
        g = i // TILE
        e, t, k = g % 2, (g // 2) % 8, g // 16
        slot = (t // 2) * 8 + ((k // 2 + t) % 2) * 4 + (t % 2) * 2 + k % 2
        want = e * 32 + slot
        pick = (lax.broadcasted_iota(jnp.int32, (quarter, 64), 1) == want).astype(jnp.bfloat16)
        col = lax.broadcasted_iota(jnp.int32, (64, 1024), 1) // TILE
        wide = (lax.broadcasted_iota(jnp.int32, (64, 1024), 0) == col).astype(jnp.bfloat16)
        same = (
            lax.broadcasted_iota(jnp.int32, (quarter, 1024), 0) % TILE
            == lax.broadcasted_iota(jnp.int32, (quarter, 1024), 1) % TILE
        )
        for h, part in enumerate((coef_hi, coef_lo)):
            chosen = jnp.dot(pick, part, preferred_element_type=jnp.float32).astype(jnp.bfloat16)
            full = jnp.dot(chosen, wide, preferred_element_type=jnp.float32)
            lift[h, pl.ds(pl.multiple_of(n * quarter, quarter), quarter), :] = jnp.where(
                same, full, 0.0
            ).astype(jnp.bfloat16)
        return 0

    with jax.named_scope("spread"):
        lax.fori_loop(0, 4, spread, 0)

    def mine(q):
        return pl.ds(pl.multiple_of(HALO + q * CHUNK + turn * PIECE, PIECE), PIECE)

    def send_fields(k, chunk):
        for dy, dc in OWNER_OFFSETS:
            y_, core_ = (y + dy) % 4, (core + dc) % 2
            q = chunk(core_)
            pltpu.make_async_remote_copy(
                src_ref=sent.at[q, pl.ds(k * 16 + (y_ * 2 + core_) * 2, 2)],
                dst_ref=fields.at[k, :, mine(q), :],
                send_sem=s2.at[k],
                recv_sem=r2.at[k, q],
                device_id=device(y_, xl, core_, row),
                device_id_type=MESH,
            ).start()
        q = chunk(core)
        pltpu.make_async_copy(
            sent.at[q, pl.ds(k * 16 + turn * 2, 2)], fields.at[k, :, mine(q), :], r2.at[k, q]
        ).start()

    def first_chunk(core_):
        return 3 * (1 - core_)

    def second_chunk(core_):
        return 3 * core_

    def send_slot(k):
        send_fields(k, second_chunk)
        if k + 1 < SLOTS_DEV:
            send_fields(k + 1, first_chunk)
        for step in range(2):
            for q in (1, 2):
                send_component(k, q, step)

    def send_component(k, q, step):
        for dy, dc in OWNER_OFFSETS:
            y_, core_ = (y + dy) % 4, (core + dc) % 2
            e = (step + core_) % 2
            pltpu.make_async_remote_copy(
                src_ref=sent.at[q, k * 16 + (y_ * 2 + core_) * 2 + e],
                dst_ref=fields.at[k, e, mine(q), :],
                send_sem=s2.at[k],
                recv_sem=rc.at[k, q - 1, step],
                device_id=device(y_, xl, core_, row),
                device_id_type=MESH,
            ).start()
        e = (step + core) % 2
        pltpu.make_async_copy(
            sent.at[q, k * 16 + turn * 2 + e], fields.at[k, e, mine(q), :], rc.at[k, q - 1, step]
        ).start()

    for q in ORDER:
        with jax.named_scope(f"wait_one#q={q}"):
            pltpu.make_async_copy(arrived.at[q], arrived.at[q], r1.at[q]).wait()

        def transform(h, _):
            rows = pl.ds(pl.multiple_of(h * TILE, TILE), TILE)
            x = arrived[q, :, rows, :].reshape(64 * TILE, M)
            for n in range(2):
                at = pl.ds(n * 512, 512)
                out = jnp.dot(lift[0, at, :], x, preferred_element_type=jnp.float32)
                out += jnp.dot(lift[1, at, :], x, preferred_element_type=jnp.float32)
                sent[q, pl.ds(n * 32, 32), rows, :] = out.astype(jnp.bfloat16).reshape(
                    32, TILE, M
                )
            return 0

        with jax.named_scope(f"transform#q={q}"):
            lax.fori_loop(0, PIECE // TILE, transform, 0)
        if q in (1, 2):
            for step in range(2):
                send_component(0, q, step)
        else:
            send_fields(0, lambda core_: q)
        if q == 0:
            send_fields(1, first_chunk)
    send_slot(1)

    for copy in loads:
        copy.wait()

    blank = pl.ds(pl.multiple_of((1 - core) * (HALO + SEG), HALO), HALO)
    for k in range(SLOTS_DEV):
        fields[k, :, blank, :] = jnp.zeros((2, HALO, M), jnp.bfloat16)
    near_block, far_block = core * 7, 1 + core * 5
    for n, (block, lane) in enumerate(
        ((near_block, B + core * 2 * B), (far_block, core * 4 * B), (near_block, core * 4 * B))
    ):
        for m in range(2):
            piece = bands[block, pl.ds(m * B, B), pl.ds(pl.multiple_of(lane, B), B)]
            edges[n, pl.ds(m * B, B), :] = piece.astype(jnp.float32).T.astype(jnp.bfloat16)

    def across_rows(left, right):
        return lax.dot_general(
            left, right, (((0,), (0,)), ((), ())), preferred_element_type=jnp.float32
        )

    def project(rows, first):
        for e in range(2):
            part = across_rows(rows[e], images[pl.ds(0, CHUNK), :])
            at = pl.ds(e * M, M)
            if first:
                total[at, :] = part
            else:
                total[at, :] += part

    def arrival(k, q):
        whole = fields.at[k, :, pl.ds(0, CHUNK), :]
        with jax.named_scope(f"wait_two#k={k}"):
            pltpu.make_async_copy(whole, whole, r2.at[k, q]).wait()

    edge_rows = pl.ds(pl.multiple_of(core * (HALO + SEG), HALO), HALO)

    def halo(k):
        to = (seg + 1 + 14 * core) % 16
        mine = pl.ds(pl.multiple_of(SEG - core * (SEG - HALO), HALO), HALO)
        return pltpu.make_async_remote_copy(
            src_ref=fields.at[k, :, mine, :],
            dst_ref=fields.at[k, :, edge_rows, :],
            send_sem=sh.at[k],
            recv_sem=rh.at[k],
            device_id=device(y, to % 2, core, to // 2),
            device_id_type=MESH,
        )

    def pass_on(k):
        arrival(k, first_chunk(core))
        halo(k).start()

    def boundary(k):
        near = pl.ds(pl.multiple_of(HALO + core * 7 * B, B), B)
        far = pl.ds(pl.multiple_of(HALO + B + core * 5 * B, B), B)
        for e in range(2):
            low = jnp.dot(edges[0], fields[k, e, near, :], preferred_element_type=jnp.float32)
            low += jnp.dot(edges[1], fields[k, e, far, :], preferred_element_type=jnp.float32)
            deep = jnp.dot(edges[2], fields[k, e, near, :], preferred_element_type=jnp.float32)
            low, deep = low.astype(jnp.bfloat16), deep.astype(jnp.bfloat16)
            at_low = pl.ds(pl.multiple_of((1 - core) * B, B), B)
            at_deep = pl.ds(pl.multiple_of(core * B, B), B)
            for m in range(2):
                columns = pl.ds(m * 2 * M + e * M, M)
                images[at_low, columns] = low[m * B : (m + 1) * B]
                images[at_deep, columns] = deep[m * B : (m + 1) * B]
        project(fields.at[k, :, edge_rows, :], True)

    def slot(k):
        own, other = core, 1 - core

        def lanes(start, e):
            return pl.ds(pl.multiple_of(start + e * M, M), M)

        def widen(q, e):
            for b in range(2):
                i = 2 * q + b
                window = fields[k, e, pl.ds(i * B, NBAND * B), :]
                w = jnp.dot(bands[i], window, preferred_element_type=jnp.float32)
                w = w.astype(jnp.bfloat16)
                images[pl.ds(i * B, B), lanes(0, e)] = w[:B]
                images[pl.ds(i * B, B), lanes(2 * M, e)] = w[B:]

        def add(chunks, e, columns):
            start, size = chunks[0] * CHUNK, len(chunks) * CHUNK
            left = fields[k, e, pl.ds(HALO + start, size), :]
            for at in columns:
                total[lanes(0, e), at] += across_rows(left, images[pl.ds(start, size), at])

        def component(q, step):
            whole(fields.at[k, 0, pl.ds(0, CHUNK), :], rc.at[k, q - 1, step])

        def first_half(*chunks):
            for q in chunks:
                widen(q, own)
            add(chunks, own, (lanes(0, own), lanes(2 * M, own)))

        def second_half(*chunks):
            for q in chunks:
                widen(q, other)
            add(chunks, own, (lanes(0, other), lanes(2 * M, other)))

        def narrow(e, at, width):
            parts[k, pl.ds(2 * e, 2), :, :, at] = (
                total[lanes(0, e), at].astype(jnp.bfloat16).reshape(2, 2, 64, width)
            )

        arrival(k, second_chunk(core))
        if k < LAST:
            pass_on(k + 1)
        halo(k).wait_recv()
        boundary(k)
        with jax.named_scope(f"component#k={k}#q=1#n=0"):
            component(1, 0)
        first_half(0)
        with jax.named_scope(f"component#k={k}#q=2#n=0"):
            component(2, 0)
        with jax.named_scope(f"first_half#k={k}"):
            first_half(1, 2, 3)
            for m in range(2):
                narrow(own, lanes(m * 2 * M, own), M)
        send_sums(k, ((own, own),))
        with jax.named_scope(f"component#k={k}#q=1#n=1"):
            component(1, 1)
        second_half(0)
        add((0,), other, (pl.ds(0, 4 * M),))
        with jax.named_scope(f"component#k={k}#q=2#n=1"):
            component(2, 1)
        with jax.named_scope(f"second_half#k={k}"):
            second_half(1, 2, 3)
            for m in range(2):
                narrow(own, lanes(m * 2 * M, other), M)
        send_sums(k, ((own, other),))
        with jax.named_scope(f"third_part#k={k}"):
            add((1, 2, 3), other, (pl.ds(0, 4 * M),))
            narrow(other, pl.ds(0, 4 * M), 4 * M)
        send_sums(k, ((other, None),))

    def send_sums(k, blocks):
        def lanes(start, e):
            if e is None:
                return pl.ds(start, WIDE)
            return pl.ds(pl.multiple_of(start + e * M, M), M)

        for rows_e, cols_e in blocks:
            planes = pl.ds(2 * rows_e, 2)

            def to_owner(dh):
                xh_ = (xh + dh) % 2
                return pltpu.make_async_remote_copy(
                    src_ref=parts.at[k, planes, xh_, :, lanes(WIDE, cols_e)],
                    dst_ref=mass_in.at[k % 2, place, planes, :, lanes(0, cols_e)],
                    send_sem=sm1.at[k, dh],
                    recv_sem=rm1.at[k % 2],
                    device_id=device(y, owner(k), core, z * 2 + xh_),
                    device_id_type=MESH,
                )

            to_owner(1).start()

            @pl.when(xl == owner(k))
            def _():
                pltpu.make_async_copy(
                    parts.at[k, planes, xh, :, lanes(WIDE, cols_e)],
                    mass_in.at[k % 2, place, planes, :, lanes(0, cols_e)],
                    rm1.at[k % 2],
                ).start()

            @pl.when(xl != owner(k))
            def _():
                to_owner(0).start()

            for dz in (1, 3, 2):
                z_ = (z + dz) % 4

                @pl.when(z_ // 2 == rows_e)
                def _():
                    pltpu.make_async_remote_copy(
                        src_ref=parts.at[k, z_, :, :, lanes(0, cols_e)],
                        dst_ref=stiff_in.at[k, 3 - dz, :, :, lanes(0, cols_e)],
                        send_sem=sk1.at[k],
                        recv_sem=rk1.at[k],
                        device_id=device(y, xl, core, z_ * 2 + xh),
                        device_id_type=MESH,
                    ).start()

    place = xh * 2 + xl

    def owner(k):
        return (k // 2 + core) % 2

    def stiff_second(k, dh):
        xh_ = (xh + dh) % 2
        return pltpu.make_async_remote_copy(
            src_ref=stiff_mid.at[k, xh_],
            dst_ref=stiff_end.at[k % 2, place],
            send_sem=sk2.at[k, dh],
            recv_sem=rk2.at[k % 2],
            device_id=device(y, owner(k), core, z * 2 + xh_),
            device_id_type=MESH,
        )

    def mass_first(k, dh):
        xh_ = (xh + dh) % 2
        return pltpu.make_async_remote_copy(
            src_ref=parts.at[k, :, xh_, :, pl.ds(WIDE, WIDE)],
            dst_ref=mass_in.at[k % 2, place],
            send_sem=sm1.at[k, dh],
            recv_sem=rm1.at[k % 2],
            device_id=device(y, owner(k), core, z * 2 + xh_),
            device_id_type=MESH,
        )

    def mass_second(k, dz):
        z_ = (z + dz) % 4
        return pltpu.make_async_remote_copy(
            src_ref=mass_mid.at[k % 2, z_],
            dst_ref=mass_end.at[k % 2, 3 - dz],
            send_sem=sm2.at[k % 2],
            recv_sem=rm2.at[k % 2],
            device_id=device(y, xl, core, z_ * 2 + xh),
            device_id_type=MESH,
        )

    def whole(ref, sem):
        pltpu.make_async_copy(ref, ref, sem).wait()

    def second(k):
        with jax.named_scope(f"wait_stiff#k={k}"):
            whole(stiff_in.at[k], rk1.at[k])
        acc = parts[k, z, :, :, pl.ds(0, WIDE)].astype(jnp.float32)
        for n in range(3):
            acc += stiff_in[k, n].astype(jnp.float32)
        stiff_mid[k] = acc.astype(jnp.bfloat16)
        stiff_second(k, 1).start()

        @pl.when(xl == owner(k))
        def _():
            pltpu.make_async_copy(
                stiff_mid.at[k, xh], stiff_end.at[k % 2, place], rk2.at[k % 2]
            ).start()
            with jax.named_scope(f"wait_mass#k={k}"):
                whole(mass_in.at[k % 2], rm1.at[k % 2])
            acc = mass_in[k % 2, 0].astype(jnp.float32)
            for n in range(1, 4):
                acc += mass_in[k % 2, n].astype(jnp.float32)
            mass_mid[k % 2] = acc.astype(jnp.bfloat16)
            for dz in (1, 3, 2):
                mass_second(k, dz).start()

        @pl.when(xl != owner(k))
        def _():
            stiff_second(k, 0).start()

    for k in range(SLOTS_DEV):
        if k + 2 < SLOTS_DEV:
            send_slot(k + 2)
        if k == 0:
            pass_on(0)
        slot(k)
        if k in (1, 2):
            second(k - 1)
    for k in range(SLOTS_DEV):
        if k + 1 not in (1, 2):
            second(k)

    for q in range(NCHUNK):
        gone = arrived.at[q, pl.ds(0, 60)]
        pltpu.make_async_copy(gone, gone, s1.at[q]).wait()
    for k in range(SLOTS_DEV):
        gone = sent.at[pl.ds(0, 4), pl.ds(0, 14)]
        pltpu.make_async_copy(gone, gone, s2.at[k]).wait()
        halo(k).wait_send()
        whole(stiff_in.at[k], sk1.at[k])
        mass_first(k, 1).wait_send()

        @pl.when(xl != owner(k))
        def _():
            mass_first(k, 0).wait_send()

    for k in range(2):
        with jax.named_scope(f"wait_end#k={k}"):
            whole(stiff_end.at[k], rk2.at[k])
            whole(mass_end.at[k], rm2.at[k])
        acc = stiff_end[k, 0].astype(jnp.float32)
        for n in range(1, 4):
            acc += stiff_end[k, n].astype(jnp.float32)
        out[0, k] = acc
        acc = mass_mid[k, z].astype(jnp.float32)
        for n in range(3):
            acc += mass_end[k, n].astype(jnp.float32)
        out[1, k] = acc

    for k in range(SLOTS_DEV):
        stiff_second(k, 1).wait_send()

        @pl.when(xl != owner(k))
        def _():
            stiff_second(k, 0).wait_send()

    for k in range(2):
        whole(mass_end.at[k], sm2.at[k])


def per_device(psi_sectors, stiff_blocks, mass_blocks, harmonic_table):
    anywhere = pl.BlockSpec(memory_space=pl.ANY)
    vmem = pl.BlockSpec(memory_space=pltpu.VMEM)
    bf16, f32 = jnp.bfloat16, jnp.float32
    dma = pltpu.SemaphoreType.DMA
    out = pl.pallas_call(
        kernel,
        out_shape=jax.ShapeDtypeStruct((2, 2, 64, 512), f32),
        in_specs=[anywhere, anywhere, anywhere, anywhere],
        out_specs=pl.BlockSpec(memory_space=pltpu.VMEM),
        scratch_shapes=[
            pltpu.VMEM((NCHUNK, 64, PIECE, M), bf16),
            pltpu.VMEM((NCHUNK, 64, PIECE, M), bf16),
            pltpu.VMEM((SLOTS_DEV, 2, SEG + 2 * HALO, M), bf16),
            pltpu.VMEM((2, 1024, 1024), bf16),
            pltpu.VMEM((8, 2 * B, NBAND * B), bf16),
            pltpu.VMEM((3, 2 * B, B), bf16),
            pltpu.VMEM((SEG, 4 * M), bf16),
            pltpu.VMEM((2 * M, 4 * M), f32),
            pltpu.VMEM((SLOTS_DEV, 4, 2, 64, 2 * WIDE), bf16),
            pltpu.VMEM((SLOTS_DEV, 3, 2, 64, WIDE), bf16),
            pltpu.VMEM((SLOTS_DEV, 2, 64, WIDE), bf16),
            pltpu.VMEM((2, 4, 64, WIDE), bf16),
            pltpu.VMEM((2, 4, 4, 64, WIDE), bf16),
            pltpu.VMEM((2, 4, 64, WIDE), bf16),
            pltpu.VMEM((2, 3, 64, WIDE), bf16),
            pltpu.SMEM((SLOTS,), jnp.int32),
            dma,
            dma((2, NBAND)),
            dma((NCHUNK,)),
            dma((NCHUNK,)),
            dma((SLOTS_DEV,)),
            dma((SLOTS_DEV, NCHUNK)),
            dma((SLOTS_DEV, 2, 2)),
            dma((SLOTS_DEV,)),
            dma((SLOTS_DEV,)),
            dma((SLOTS_DEV,)),
            dma((SLOTS_DEV,)),
            dma((SLOTS_DEV, 2)),
            dma((2,)),
            dma((SLOTS_DEV, 2)),
            dma((2,)),
            dma((2,)),
            dma((2,)),
        ],
        compiler_params=pltpu.CompilerParams(
            collective_id=0, has_side_effects=True, vmem_limit_bytes=52 * 1024 * 1024
        ),
        name="reduce_sectors",
    )(psi_sectors, stiff_blocks, mass_blocks, harmonic_table)
    return out[0], out[1]


def solution(mesh):
    placed = (P("sector", "row", None), P("row", None, None, None), P("row", None, None, None), P())
    return jax.shard_map(
        per_device,
        mesh=mesh,
        in_specs=placed,
        out_specs=(P("sector", "row", None), P("sector", "row", None)),
        check_vma=False,
    )
```

```python
import functools
import math

import jax
import jax.numpy as jnp
from jax import lax
from jax.experimental import pallas as pl
from jax.experimental.pallas import tpu as pltpu
from jax.sharding import PartitionSpec as P

MESH = pl.DeviceIdType.MESH
B = 128
M = 256
NBAND = 5
ROWS_DEV = 2048
SEG = 1024
CHUNK = 256
NCHUNK = 4
PIECE = 32
TILE = 16
SLOTS_DEV = 4
LAST = SLOTS_DEV - 1
ORDER = (3, 0, 1, 2)
HALO = 256
WIDE = 512
SECTORS = 64
SLOTS = 32
SECTOR_OFFSETS = tuple(
    (dy, dx, dc) for dy in (2, 1, 3, 0) for dx in (1, 0) for dc in (0, 1) if dy or dx or dc
)
OWNER_OFFSETS = tuple((dy, dc) for dy in (2, 1, 3, 0) for dc in (0, 1) if dy or dc)


def coefficients(table):
    shape = (2 * SLOTS, SECTORS)
    line = lax.broadcasted_iota(jnp.int32, shape, 0)
    sector = lax.broadcasted_iota(jnp.int32, shape, 1)
    pair = jnp.zeros(shape, jnp.int32)
    for j in range(SLOTS):
        pair = jnp.where(line % SLOTS == j, table[j], pair)
    first = line < SLOTS
    zero = pair == 0
    freq = jnp.where(jnp.logical_and(zero, jnp.logical_not(first)), SECTORS // 2, pair)
    shift = jnp.where(jnp.logical_or(first, zero), 0, 3 * SECTORS // 4)
    phase = (freq * sector + shift) % SECTORS
    wave = jnp.cos(phase.astype(jnp.float32) * (2.0 * math.pi / SECTORS))
    return jnp.where(zero, math.sqrt(1.0 / SECTORS), math.sqrt(2.0 / SECTORS)) * wave


def kernel(
    psi, stiff, mass, table_in, out,
    arrived, sent, fields, lift, bands, edges, images, total, parts,
    stiff_in, stiff_mid, stiff_end, mass_in, mass_mid, mass_end, table, table_sem,
    load_sem, s1, r1, s2, r2, rc, sh, rh, sk1, rk1, sk2, rk2, sm1, rm1, sm2, rm2,
):
    sec = lax.axis_index("sector")
    row = lax.axis_index("row")
    y, xl, core = sec // 4, (sec // 2) % 2, sec % 2
    turn = y * 2 + core
    seg = row * 2 + xl
    z, xh = row // 2, row % 2

    def device(y_, xl_, core_, row_):
        return {"sector": y_ * 4 + xl_ * 2 + core_, "row": row_}

    barrier = pltpu.get_barrier_semaphore()
    count = 0
    for dy, dx, dc in SECTOR_OFFSETS:
        pl.semaphore_signal(
            barrier, inc=1, device_id_type=MESH,
            device_id=device((y + dy) % 4, (xl + dx) % 2, (core + dc) % 2, row),
        )
        count += 1
    for dr in range(1, 8):
        for dx in range(2):
            pl.semaphore_signal(
                barrier, inc=1, device_id_type=MESH,
                device_id=device(y, (xl + dx) % 2, core, (row + dr) % 8),
            )
            count += 1
    table_copy = pltpu.make_async_copy(table_in, table, table_sem)
    table_copy.start()
    loads = []
    for m, src in enumerate((stiff, mass)):
        for k in range(NBAND):
            copy = pltpu.make_async_copy(
                src.at[pl.ds(pl.multiple_of(xl * 8, 8), 8), k],
                bands.at[:, pl.ds(m * B, B), pl.ds(k * B, B)],
                load_sem.at[m, k],
            )
            copy.start()
            loads.append(copy)

    with jax.named_scope("barrier"):
        pl.semaphore_wait(barrier, count)

    def rows_of(xl_, turn_, q):
        return pl.ds(pl.multiple_of(xl_ * SEG + q * CHUNK + turn_ * PIECE, PIECE), PIECE)

    for q in ORDER:
        for dy, dx, dc in SECTOR_OFFSETS:
            y_, xl_, core_ = (y + dy) % 4, (xl + dx) % 2, (core + dc) % 2
            pltpu.make_async_remote_copy(
                src_ref=psi.at[:, rows_of(xl_, y_ * 2 + core_, q), :],
                dst_ref=arrived.at[q, pl.ds(sec * 4, 4)],
                send_sem=s1.at[q],
                recv_sem=r1.at[q],
                device_id=device(y_, xl_, core_, row),
                device_id_type=MESH,
            ).start()
        pltpu.make_async_copy(
            psi.at[:, rows_of(xl, turn, q), :], arrived.at[q, pl.ds(sec * 4, 4)], r1.at[q]
        ).start()

    table_copy.wait()
    coef = coefficients(table)
    coef_hi = coef.astype(jnp.bfloat16)
    coef_lo = (coef - coef_hi.astype(jnp.float32)).astype(jnp.bfloat16)
    quarter = 256

    def spread(n, _):
        i = lax.broadcasted_iota(jnp.int32, (quarter, 64), 0) + n * quarter
        g = i // TILE
        e, t, k = g % 2, (g // 2) % 8, g // 16
        slot = (t // 2) * 8 + ((k // 2 + t) % 2) * 4 + (t % 2) * 2 + k % 2
        want = e * 32 + slot
        pick = (lax.broadcasted_iota(jnp.int32, (quarter, 64), 1) == want).astype(jnp.bfloat16)
        col = lax.broadcasted_iota(jnp.int32, (64, 1024), 1) // TILE
        wide = (lax.broadcasted_iota(jnp.int32, (64, 1024), 0) == col).astype(jnp.bfloat16)
        same = (
            lax.broadcasted_iota(jnp.int32, (quarter, 1024), 0) % TILE
            == lax.broadcasted_iota(jnp.int32, (quarter, 1024), 1) % TILE
        )
        for h, part in enumerate((coef_hi, coef_lo)):
            chosen = jnp.dot(pick, part, preferred_element_type=jnp.float32).astype(jnp.bfloat16)
            full = jnp.dot(chosen, wide, preferred_element_type=jnp.float32)
            lift[h, pl.ds(pl.multiple_of(n * quarter, quarter), quarter), :] = jnp.where(
                same, full, 0.0
            ).astype(jnp.bfloat16)
        return 0

    with jax.named_scope("spread"):
        lax.fori_loop(0, 4, spread, 0)

    def mine(q):
        return pl.ds(pl.multiple_of(HALO + q * CHUNK + turn * PIECE, PIECE), PIECE)

    def send_fields(k, chunk):
        for dy, dc in OWNER_OFFSETS:
            y_, core_ = (y + dy) % 4, (core + dc) % 2
            q = chunk(core_)
            pltpu.make_async_remote_copy(
                src_ref=sent.at[q, pl.ds(k * 16 + (y_ * 2 + core_) * 2, 2)],
                dst_ref=fields.at[k, :, mine(q), :],
                send_sem=s2.at[k],
                recv_sem=r2.at[k, q],
                device_id=device(y_, xl, core_, row),
                device_id_type=MESH,
            ).start()
        q = chunk(core)
        pltpu.make_async_copy(
            sent.at[q, pl.ds(k * 16 + turn * 2, 2)], fields.at[k, :, mine(q), :], r2.at[k, q]
        ).start()

    def first_chunk(core_):
        return 3 * (1 - core_)

    def second_chunk(core_):
        return 3 * core_

    def send_slot(k):
        send_fields(k, second_chunk)
        if k + 1 < SLOTS_DEV:
            send_fields(k + 1, first_chunk)
        for step in range(2):
            for q in (1, 2):
                send_component(k, q, step)

    def send_component(k, q, step):
        for dy, dc in OWNER_OFFSETS:
            y_, core_ = (y + dy) % 4, (core + dc) % 2
            e = (step + core_) % 2
            pltpu.make_async_remote_copy(
                src_ref=sent.at[q, k * 16 + (y_ * 2 + core_) * 2 + e],
                dst_ref=fields.at[k, e, mine(q), :],
                send_sem=s2.at[k],
                recv_sem=rc.at[k, q - 1, step],
                device_id=device(y_, xl, core_, row),
                device_id_type=MESH,
            ).start()
        e = (step + core) % 2
        pltpu.make_async_copy(
            sent.at[q, k * 16 + turn * 2 + e], fields.at[k, e, mine(q), :], rc.at[k, q - 1, step]
        ).start()

    for q in ORDER:
        with jax.named_scope(f"wait_one#q={q}"):
            pltpu.make_async_copy(arrived.at[q], arrived.at[q], r1.at[q]).wait()

        def transform(h, _):
            rows = pl.ds(pl.multiple_of(h * TILE, TILE), TILE)
            x = arrived[q, :, rows, :].reshape(64 * TILE, M)
            for n in range(2):
                at = pl.ds(n * 512, 512)
                out = jnp.dot(lift[0, at, :], x, preferred_element_type=jnp.float32)
                out += jnp.dot(lift[1, at, :], x, preferred_element_type=jnp.float32)
                sent[q, pl.ds(n * 32, 32), rows, :] = out.astype(jnp.bfloat16).reshape(
                    32, TILE, M
                )
            return 0

        with jax.named_scope(f"transform#q={q}"):
            lax.fori_loop(0, PIECE // TILE, transform, 0)
        if q in (1, 2):
            for step in range(2):
                send_component(0, q, step)
        else:
            send_fields(0, lambda core_: q)
        if q == 0:
            send_fields(1, first_chunk)
    send_slot(1)

    for copy in loads:
        copy.wait()

    blank = pl.ds(pl.multiple_of((1 - core) * (HALO + SEG), HALO), HALO)
    for k in range(SLOTS_DEV):
        fields[k, :, blank, :] = jnp.zeros((2, HALO, M), jnp.bfloat16)
    near_block, far_block = core * 7, 1 + core * 5
    for n, (block, lane) in enumerate(
        ((near_block, B + core * 2 * B), (far_block, core * 4 * B), (near_block, core * 4 * B))
    ):
        for m in range(2):
            piece = bands[block, pl.ds(m * B, B), pl.ds(pl.multiple_of(lane, B), B)]
            edges[n, pl.ds(m * B, B), :] = piece.astype(jnp.float32).T.astype(jnp.bfloat16)

    def across_rows(left, right):
        return lax.dot_general(
            left, right, (((0,), (0,)), ((), ())), preferred_element_type=jnp.float32
        )

    def project(rows, first):
        for e in range(2):
            part = across_rows(rows[e], images[pl.ds(0, CHUNK), :])
            at = pl.ds(e * M, M)
            if first:
                total[at, :] = part
            else:
                total[at, :] += part

    def arrival(k, q):
        whole = fields.at[k, :, pl.ds(0, CHUNK), :]
        with jax.named_scope(f"wait_two#k={k}"):
            pltpu.make_async_copy(whole, whole, r2.at[k, q]).wait()

    edge_rows = pl.ds(pl.multiple_of(core * (HALO + SEG), HALO), HALO)

    def halo(k):
        to = (seg + 1 + 14 * core) % 16
        mine = pl.ds(pl.multiple_of(SEG - core * (SEG - HALO), HALO), HALO)
        return pltpu.make_async_remote_copy(
            src_ref=fields.at[k, :, mine, :],
            dst_ref=fields.at[k, :, edge_rows, :],
            send_sem=sh.at[k],
            recv_sem=rh.at[k],
            device_id=device(y, to % 2, core, to // 2),
            device_id_type=MESH,
        )

    def pass_on(k):
        arrival(k, first_chunk(core))
        halo(k).start()

    def boundary(k):
        near = pl.ds(pl.multiple_of(HALO + core * 7 * B, B), B)
        far = pl.ds(pl.multiple_of(HALO + B + core * 5 * B, B), B)
        for e in range(2):
            low = jnp.dot(edges[0], fields[k, e, near, :], preferred_element_type=jnp.float32)
            low += jnp.dot(edges[1], fields[k, e, far, :], preferred_element_type=jnp.float32)
            deep = jnp.dot(edges[2], fields[k, e, near, :], preferred_element_type=jnp.float32)
            low, deep = low.astype(jnp.bfloat16), deep.astype(jnp.bfloat16)
            at_low = pl.ds(pl.multiple_of((1 - core) * B, B), B)
            at_deep = pl.ds(pl.multiple_of(core * B, B), B)
            for m in range(2):
                columns = pl.ds(m * 2 * M + e * M, M)
                images[at_low, columns] = low[m * B : (m + 1) * B]
                images[at_deep, columns] = deep[m * B : (m + 1) * B]
        project(fields.at[k, :, edge_rows, :], True)

    def slot(k):
        own, other = core, 1 - core

        def lanes(start, e):
            return pl.ds(pl.multiple_of(start + e * M, M), M)

        def widen(q, e):
            for b in range(2):
                i = 2 * q + b
                window = fields[k, e, pl.ds(i * B, NBAND * B), :]
                w = jnp.dot(bands[i], window, preferred_element_type=jnp.float32)
                w = w.astype(jnp.bfloat16)
                images[pl.ds(i * B, B), lanes(0, e)] = w[:B]
                images[pl.ds(i * B, B), lanes(2 * M, e)] = w[B:]

        def add(chunks, e, columns):
            start, size = chunks[0] * CHUNK, len(chunks) * CHUNK
            left = fields[k, e, pl.ds(HALO + start, size), :]
            for at in columns:
                total[lanes(0, e), at] += across_rows(left, images[pl.ds(start, size), at])

        def component(q, step):
            whole(fields.at[k, 0, pl.ds(0, CHUNK), :], rc.at[k, q - 1, step])

        def first_half(*chunks):
            for q in chunks:
                widen(q, own)
            add(chunks, own, (lanes(0, own), lanes(2 * M, own)))

        def second_half(*chunks):
            for q in chunks:
                widen(q, other)
            add(chunks, own, (lanes(0, other), lanes(2 * M, other)))

        def narrow(e, at, width):
            parts[k, pl.ds(2 * e, 2), :, :, at] = (
                total[lanes(0, e), at].astype(jnp.bfloat16).reshape(2, 2, 64, width)
            )

        arrival(k, second_chunk(core))
        if k < LAST:
            pass_on(k + 1)
        halo(k).wait_recv()
        boundary(k)
        with jax.named_scope(f"component#k={k}#q=1#n=0"):
            component(1, 0)
        first_half(0)
        with jax.named_scope(f"component#k={k}#q=2#n=0"):
            component(2, 0)
        with jax.named_scope(f"first_half#k={k}"):
            first_half(1, 2, 3)
            for m in range(2):
                narrow(own, lanes(m * 2 * M, own), M)
        send_sums(k, ((own, own),))
        with jax.named_scope(f"component#k={k}#q=1#n=1"):
            component(1, 1)
        second_half(0)
        add((0,), other, (pl.ds(0, 4 * M),))
        with jax.named_scope(f"component#k={k}#q=2#n=1"):
            component(2, 1)
        with jax.named_scope(f"second_half#k={k}"):
            second_half(1, 2, 3)
            for m in range(2):
                narrow(own, lanes(m * 2 * M, other), M)
        send_sums(k, ((own, other),))
        with jax.named_scope(f"third_part#k={k}"):
            add((1, 2, 3), other, (pl.ds(0, 4 * M),))
            narrow(other, pl.ds(0, 4 * M), 4 * M)
        send_sums(k, ((other, None),))

    def send_sums(k, blocks):
        def lanes(start, e):
            if e is None:
                return pl.ds(start, WIDE)
            return pl.ds(pl.multiple_of(start + e * M, M), M)

        for rows_e, cols_e in blocks:
            planes = pl.ds(2 * rows_e, 2)

            def to_owner(dh):
                xh_ = (xh + dh) % 2
                return pltpu.make_async_remote_copy(
                    src_ref=parts.at[k, planes, xh_, :, lanes(WIDE, cols_e)],
                    dst_ref=mass_in.at[k % 2, place, planes, :, lanes(0, cols_e)],
                    send_sem=sm1.at[k, dh],
                    recv_sem=rm1.at[k % 2],
                    device_id=device(y, owner(k), core, z * 2 + xh_),
                    device_id_type=MESH,
                )


            @pl.when(xl == owner(k))
            def _():
                pltpu.make_async_copy(
                    parts.at[k, planes, xh, :, lanes(WIDE, cols_e)],
                    mass_in.at[k % 2, place, planes, :, lanes(0, cols_e)],
                    rm1.at[k % 2],
                ).start()

            @pl.when(xl != owner(k))
            def _():
                to_owner(0).start()

            to_owner(1).start()

            for dz in (1, 3, 2):
                z_ = (z + dz) % 4

                @pl.when(z_ // 2 == rows_e)
                def _():
                    pltpu.make_async_remote_copy(
                        src_ref=parts.at[k, z_, :, :, lanes(0, cols_e)],
                        dst_ref=stiff_in.at[k, 3 - dz, :, :, lanes(0, cols_e)],
                        send_sem=sk1.at[k],
                        recv_sem=rk1.at[k],
                        device_id=device(y, xl, core, z_ * 2 + xh),
                        device_id_type=MESH,
                    ).start()

    place = xh * 2 + xl

    def owner(k):
        return (k // 2 + core) % 2

    def stiff_second(k, dh):
        xh_ = (xh + dh) % 2
        return pltpu.make_async_remote_copy(
            src_ref=stiff_mid.at[k, xh_],
            dst_ref=stiff_end.at[k % 2, place],
            send_sem=sk2.at[k, dh],
            recv_sem=rk2.at[k % 2],
            device_id=device(y, owner(k), core, z * 2 + xh_),
            device_id_type=MESH,
        )

    def mass_first(k, dh):
        xh_ = (xh + dh) % 2
        return pltpu.make_async_remote_copy(
            src_ref=parts.at[k, :, xh_, :, pl.ds(WIDE, WIDE)],
            dst_ref=mass_in.at[k % 2, place],
            send_sem=sm1.at[k, dh],
            recv_sem=rm1.at[k % 2],
            device_id=device(y, owner(k), core, z * 2 + xh_),
            device_id_type=MESH,
        )

    def mass_second(k, dz):
        z_ = (z + dz) % 4
        return pltpu.make_async_remote_copy(
            src_ref=mass_mid.at[k % 2, z_],
            dst_ref=mass_end.at[k % 2, 3 - dz],
            send_sem=sm2.at[k % 2],
            recv_sem=rm2.at[k % 2],
            device_id=device(y, xl, core, z_ * 2 + xh),
            device_id_type=MESH,
        )

    def whole(ref, sem):
        pltpu.make_async_copy(ref, ref, sem).wait()

    def second(k):
        with jax.named_scope(f"wait_stiff#k={k}"):
            whole(stiff_in.at[k], rk1.at[k])
        acc = parts[k, z, :, :, pl.ds(0, WIDE)].astype(jnp.float32)
        for n in range(3):
            acc += stiff_in[k, n].astype(jnp.float32)
        stiff_mid[k] = acc.astype(jnp.bfloat16)
        stiff_second(k, 1).start()

        @pl.when(xl == owner(k))
        def _():
            pltpu.make_async_copy(
                stiff_mid.at[k, xh], stiff_end.at[k % 2, place], rk2.at[k % 2]
            ).start()
            with jax.named_scope(f"wait_mass#k={k}"):
                whole(mass_in.at[k % 2], rm1.at[k % 2])
            acc = mass_in[k % 2, 0].astype(jnp.float32)
            for n in range(1, 4):
                acc += mass_in[k % 2, n].astype(jnp.float32)
            mass_mid[k % 2] = acc.astype(jnp.bfloat16)
            for dz in (1, 3, 2):
                mass_second(k, dz).start()

        @pl.when(xl != owner(k))
        def _():
            stiff_second(k, 0).start()

    for k in range(SLOTS_DEV):
        if k + 2 < SLOTS_DEV:
            send_slot(k + 2)
        if k == 0:
            pass_on(0)
        slot(k)
        if k in (1, 2):
            second(k - 1)
    for k in range(SLOTS_DEV):
        if k + 1 not in (1, 2):
            second(k)

    for q in range(NCHUNK):
        gone = arrived.at[q, pl.ds(0, 60)]
        pltpu.make_async_copy(gone, gone, s1.at[q]).wait()
    for k in range(SLOTS_DEV):
        gone = sent.at[pl.ds(0, 4), pl.ds(0, 14)]
        pltpu.make_async_copy(gone, gone, s2.at[k]).wait()
        halo(k).wait_send()
        whole(stiff_in.at[k], sk1.at[k])
        mass_first(k, 1).wait_send()

        @pl.when(xl != owner(k))
        def _():
            mass_first(k, 0).wait_send()

    for k in range(2):
        with jax.named_scope(f"wait_end#k={k}"):
            whole(stiff_end.at[k], rk2.at[k])
            whole(mass_end.at[k], rm2.at[k])
        acc = stiff_end[k, 0].astype(jnp.float32)
        for n in range(1, 4):
            acc += stiff_end[k, n].astype(jnp.float32)
        out[0, k] = acc
        acc = mass_mid[k, z].astype(jnp.float32)
        for n in range(3):
            acc += mass_end[k, n].astype(jnp.float32)
        out[1, k] = acc

    for k in range(SLOTS_DEV):
        stiff_second(k, 1).wait_send()

        @pl.when(xl != owner(k))
        def _():
            stiff_second(k, 0).wait_send()

    for k in range(2):
        whole(mass_end.at[k], sm2.at[k])


def per_device(psi_sectors, stiff_blocks, mass_blocks, harmonic_table):
    anywhere = pl.BlockSpec(memory_space=pl.ANY)
    vmem = pl.BlockSpec(memory_space=pltpu.VMEM)
    bf16, f32 = jnp.bfloat16, jnp.float32
    dma = pltpu.SemaphoreType.DMA
    out = pl.pallas_call(
        kernel,
        out_shape=jax.ShapeDtypeStruct((2, 2, 64, 512), f32),
        in_specs=[anywhere, anywhere, anywhere, anywhere],
        out_specs=pl.BlockSpec(memory_space=pltpu.VMEM),
        scratch_shapes=[
            pltpu.VMEM((NCHUNK, 64, PIECE, M), bf16),
            pltpu.VMEM((NCHUNK, 64, PIECE, M), bf16),
            pltpu.VMEM((SLOTS_DEV, 2, SEG + 2 * HALO, M), bf16),
            pltpu.VMEM((2, 1024, 1024), bf16),
            pltpu.VMEM((8, 2 * B, NBAND * B), bf16),
            pltpu.VMEM((3, 2 * B, B), bf16),
            pltpu.VMEM((SEG, 4 * M), bf16),
            pltpu.VMEM((2 * M, 4 * M), f32),
            pltpu.VMEM((SLOTS_DEV, 4, 2, 64, 2 * WIDE), bf16),
            pltpu.VMEM((SLOTS_DEV, 3, 2, 64, WIDE), bf16),
            pltpu.VMEM((SLOTS_DEV, 2, 64, WIDE), bf16),
            pltpu.VMEM((2, 4, 64, WIDE), bf16),
            pltpu.VMEM((2, 4, 4, 64, WIDE), bf16),
            pltpu.VMEM((2, 4, 64, WIDE), bf16),
            pltpu.VMEM((2, 3, 64, WIDE), bf16),
            pltpu.SMEM((SLOTS,), jnp.int32),
            dma,
            dma((2, NBAND)),
            dma((NCHUNK,)),
            dma((NCHUNK,)),
            dma((SLOTS_DEV,)),
            dma((SLOTS_DEV, NCHUNK)),
            dma((SLOTS_DEV, 2, 2)),
            dma((SLOTS_DEV,)),
            dma((SLOTS_DEV,)),
            dma((SLOTS_DEV,)),
            dma((SLOTS_DEV,)),
            dma((SLOTS_DEV, 2)),
            dma((2,)),
            dma((SLOTS_DEV, 2)),
            dma((2,)),
            dma((2,)),
            dma((2,)),
        ],
        compiler_params=pltpu.CompilerParams(
            collective_id=0, has_side_effects=True, vmem_limit_bytes=52 * 1024 * 1024
        ),
        name="reduce_sectors",
    )(psi_sectors, stiff_blocks, mass_blocks, harmonic_table)
    return out[0], out[1]


def solution(mesh):
    placed = (P("sector", "row", None), P("row", None, None, None), P("row", None, None, None), P())
    return jax.shard_map(
        per_device,
        mesh=mesh,
        in_specs=placed,
        out_specs=(P("sector", "row", None), P("sector", "row", None)),
        check_vma=False,
    )
```
